32 devices in a mesh: band: 4 (over y, x), grid: 8 (over z, core).
Axes of the slice: x: 2, y: 2, z: 4, core: 2. Of those that a mesh axis runs over, the one named last changes fastest.
Arguments:
- coefficients: bfloat16 [256, 18, 2048], P('grid', None, 'band'), may hold values from -0.125 to 0.125
- occupation: int32 [2048], P('band'), may hold values from 0 to 8
- shapes: bfloat16 [171, 32768], replicated, may hold values from -1.5 to 1.5
- corners: int32 [3, 256], replicated, may hold values from 0 to 256, as said below
Outputs:
- density: float32 [256, 288, 288], P('grid')
The draws below stay inside these ranges and needn't reach their ends.
Inputs may be any that keep to these rules, and one draw needn't show every extreme that they name: Every box lies inside the grid. Counting atoms by the slab floor(corners[0, a] / 32), no slab holds more than 64 atoms, some slab holds exactly 64, and every slab holds at least 16.
All inputs are finite; a program needn't handle non-finite values.
Results may differ from the reference program's by a relative error of at most 0.0029.
Values may be sent and summed in bfloat16 or wider, within the bound.
A program may use at most 192 MiB of HBM per device.

```python
import jax
import jax.numpy as jnp
import numpy as np
from jax import lax

NPROJ = 18
BOX = 32
ZS = 32
NY = 288
NX = 288
AT_DEV = 32
NPAIR = 171
ATOMS = 256
BANDS = 2048
NZ = 256
N_GRID = 8


def draw_corners(key, part):
    key_order = jax.random.fold_in(key, 11)
    key_depth = jax.random.fold_in(key, 12)
    key_row = jax.random.fold_in(key, 13)
    key_column = jax.random.fold_in(key, 14)
    key_atoms = jax.random.fold_in(key, 15)
    slab_order = jax.random.permutation(key_order, N_GRID)
    quarter = N_GRID // 4
    ranks = jnp.arange(N_GRID, dtype=jnp.int32)
    loads = jnp.where(ranks < quarter, 2 * AT_DEV, jnp.where(ranks < 2 * quarter, AT_DEV, AT_DEV // 2)).astype(jnp.int32)
    bounds = jnp.cumsum(loads).astype(jnp.int32)
    positions = jnp.arange(ATOMS, dtype=jnp.int32)
    atom_rank = jnp.sum((positions[:, None] >= bounds[None, :]).astype(jnp.int32), axis=1)
    slab = slab_order[atom_rank].astype(jnp.int32)
    top = jnp.where(slab == N_GRID - 1, ZS - BOX + 1, ZS).astype(jnp.int32)
    local = jax.random.randint(key_depth, (ATOMS,), 0, top).astype(jnp.int32)
    depth = slab * ZS + local
    row_start = jax.random.randint(key_row, (ATOMS,), 0, NY - BOX + 1).astype(jnp.int32)
    column_start = jax.random.randint(key_column, (ATOMS,), 0, NX - BOX + 1).astype(jnp.int32)
    stacked = jnp.stack([depth, row_start, column_start]).astype(jnp.int32)
    order = jax.random.permutation(key_atoms, ATOMS)
    return stacked[:, order]


def with_ends(drawn, stream_key, low, high):
    spot = [jax.random.randint(jax.random.fold_in(stream_key, axis), (), 0, length) for axis, length in enumerate(drawn.shape)]
    main_axis = drawn.shape.index(max(drawn.shape))
    neighbour = spot[:main_axis] + [(spot[main_axis] + 1) % drawn.shape[main_axis]] + spot[main_axis + 1:]
    return drawn.at[tuple(spot)].set(low).at[tuple(neighbour)].set(high)


def steps_of(stream_key, shape, pieces, smallest, top_value):
    level, own = 1.0, jax.random.fold_in(stream_key, 6)
    for axis_at, parts in pieces:
        draws = jnp.exp(jax.random.uniform(jax.random.fold_in(own, axis_at), (parts,), jnp.float32, smallest / len(pieces), top_value / len(pieces)))
        level = level * jnp.repeat(draws, shape[axis_at] // parts).reshape([-1 if axis == axis_at else 1 for axis in range(len(shape))])
    return level


def normal_values(key, dims, width, bound, pieces=(), kind=jnp.bfloat16):
    result = width * jax.random.normal(key, dims, jnp.float32)
    if pieces:
        result = result * steps_of(key, dims, pieces, -0.22, 0.18)
    return jnp.clip(result, -bound, bound).astype(kind)


def setup_inputs(seed: int = 0) -> dict:
    streams_of = jax.random.split(jax.random.key(seed), 5)
    coefficients = normal_values(streams_of[0], (ATOMS, NPROJ, BANDS), BANDS ** -0.5, 0.125, ((0, 8), (2, 4)))
    occupation = with_ends(jax.random.randint(streams_of[1], (BANDS,), 0, 9), jax.random.fold_in(streams_of[1], 1), 0, 8).astype(jnp.int32)
    shapes = normal_values(streams_of[2], (NPAIR, BOX * BOX * BOX), NPROJ ** -0.5, 1.5)
    corners = draw_corners(jax.random.fold_in(streams_of[4], 71), 0)
    return {"coefficients": coefficients, "occupation": occupation, "shapes": shapes, "corners": corners}


def fold_table(count):
    table = np.zeros((count * count, count * (count + 1) // 2), np.float32)
    column = 0
    for first in range(count):
        for second in range(first, count):
            table[first * count + second, column] = 1.0
            table[second * count + first, column] = 1.0
            column = column + 1
    return table


def occupancy(coefficients, occupation):
    weighted = coefficients.astype(jnp.float32) * (occupation.astype(jnp.float32) * 0.25)[None, None, :]
    full = jnp.einsum("aib,ajb->aij", weighted, coefficients.astype(jnp.float32), precision=lax.Precision.HIGHEST)
    count = coefficients.shape[1]
    flat = full.reshape(coefficients.shape[0], count * count)
    return jnp.dot(flat, jnp.asarray(fold_table(count)), precision=lax.Precision.HIGHEST)


def reference(coefficients, occupation, shapes, corners):
    packed = occupancy(coefficients, occupation).astype(jnp.bfloat16)
    start_grid = jnp.zeros((NZ, NY, NX), jnp.float32)

    def place(grid, item):
        row, corner = item
        box = jnp.dot(row[None, :], shapes, preferred_element_type=jnp.float32).reshape(BOX, BOX, BOX)
        start = (corner[0], corner[1], corner[2])
        region = lax.dynamic_slice(grid, start, (BOX, BOX, BOX))
        return lax.dynamic_update_slice(grid, region + box, start), None

    density, unused = lax.scan(place, start_grid, (packed, corners.T.astype(jnp.int32)))
    return density
```

```python
import functools

import jax
import jax.numpy as jnp
import numpy as np
from jax import lax
from jax.experimental import pallas as pl
from jax.experimental.pallas import tpu as pltpu
from jax.sharding import PartitionSpec as P

BOX = 32
ZS = 32
NY = 288
NX = 288
LANES = 128
STEP = LANES - BOX


def fold_table(count):
    table = np.zeros((count * count, count * (count + 1) // 2), np.float32)
    column = 0
    for first in range(count):
        for second in range(first, count):
            table[first * count + second, column] = 1.0
            table[second * count + first, column] = 1.0
            column = column + 1
    return table


def occupancy(coefficients, occupation):
    weight = occupation.astype(jnp.float32) * 0.25
    weighted = coefficients.astype(jnp.float32) * weight[None, None, :]
    high = lax.reduce_precision(weighted, 8, 7)
    low = (weighted - high).astype(jnp.bfloat16)
    high = high.astype(jnp.bfloat16)
    pairs = functools.partial(jnp.einsum, "aib,ajb->aij", preferred_element_type=jnp.float32)
    full = pairs(high, coefficients) + pairs(low, coefficients)
    count = coefficients.shape[1]
    flat = full.reshape(coefficients.shape[0], count * count)
    return jnp.dot(flat, jnp.asarray(fold_table(count)), precision=lax.Precision.HIGHEST)


WINDOWS = (NX - BOX) // STEP + 1
TILES = -(-NX // LANES)
TAIL = NX % LANES
DEEP = 4
CHUNKS = ZS // DEEP
PAD = 8 * DEEP
PIECES = 4
UNROLL = 16


def place_kernel(
    slots, stride, packed_ref, corners_ref, shapes_ref, out_ref,
    shp, boxes, acc, stage, tail, table, words, shape_sem, word_sem, out_sem,
):
    slab = lax.axis_index("grid")
    atoms = packed_ref.shape[0]
    columns = shapes_ref.shape[1]
    piece = columns // PIECES
    count = 2 * slots

    def shape_copy(j):
        cols = pl.ds(j * piece, piece)
        return pltpu.make_async_copy(shapes_ref.at[:, cols], shp.at[:, cols], shape_sem.at[j])

    for j in range(PIECES):
        shape_copy(j).start()

    depth = corners_ref[0:1, :]
    owner = lax.shift_right_logical(depth, ZS.bit_length() - 1)
    local = depth - owner * ZS
    own = owner == slab
    below = jnp.logical_and(owner == slab - 1, local > 0)
    index = lax.broadcasted_iota(jnp.int32, (1, atoms), 1)
    key = jnp.where(own, local, jnp.where(below, 2 * ZS - local, 2 * ZS)) * atoms + index
    key = key.astype(jnp.float32)
    slot_rows = []
    for a in range(atoms // LANES):
        mine = key[:, a * LANES : (a + 1) * LANES]
        rank = jnp.zeros((1, LANES), jnp.float32)
        for b in range(atoms // LANES):
            other = jnp.broadcast_to(key[:, b * LANES : (b + 1) * LANES], (LANES, LANES)).T
            rank = rank + jnp.sum((other < mine).astype(jnp.float32), axis=0, keepdims=True)
        slot_rows.append(rank)
    slot_of = jnp.concatenate(slot_rows, axis=1).astype(jnp.int32)
    hot = lax.broadcasted_iota(jnp.int32, (count, atoms), 0) == slot_of
    hot = hot.astype(jnp.float32).astype(jnp.bfloat16)
    rows = jnp.dot(hot, packed_ref[...], preferred_element_type=jnp.float32).astype(jnp.bfloat16)

    start = jnp.where(own, -local, ZS - local)
    line = lax.broadcasted_iota(jnp.int32, (8, atoms), 0)
    traits = jnp.where(line == 0, corners_ref[1:2, :], jnp.where(line == 1, corners_ref[2:3, :], start))
    traits = traits.astype(jnp.float32).astype(jnp.bfloat16)
    traits = lax.dot_general(traits, hot, (((1,), (1,)), ((), ())), preferred_element_type=jnp.float32)
    traits = traits.astype(jnp.int32)
    row, column, start = traits[0:1, :], traits[1:2, :], traits[2:3, :]
    window = jnp.zeros_like(column)
    for t in range(1, WINDOWS):
        window = window + (column >= t * STEP).astype(jnp.int32)
    source = (PAD + start * 8) * stride + lax.broadcasted_iota(jnp.int32, (1, count), 1)
    target = window * NY + row
    turn = lax.bitwise_and(column + 32 * row, LANES - 1)
    line = lax.broadcasted_iota(jnp.int32, (8, count), 0)
    table[0:8, :] = jnp.where(line == 0, source, jnp.where(line == 1, target, turn))
    bound = lax.broadcasted_iota(jnp.int32, (CHUNKS, atoms), 0) * DEEP
    near = jnp.sum(jnp.where(jnp.logical_and(own, local < bound + DEEP), 1.0, 0.0), axis=1, keepdims=True)
    far = jnp.sum(jnp.where(jnp.logical_and(below, local > bound), 1.0, 0.0), axis=1, keepdims=True)
    side = lax.broadcasted_iota(jnp.int32, (CHUNKS, count), 1)
    table[8 : 8 + CHUNKS, :] = jnp.where(side == 0, near, far).astype(jnp.int32)
    word_copy = pltpu.make_async_copy(table, words, word_sem)
    word_copy.start()

    zero = jnp.zeros((8, LANES), jnp.float32)
    for edge in (0, PAD + columns // LANES):
        def clear_edge(i, carry):
            for u in range(8):
                boxes[pl.ds(edge * stride + pl.multiple_of(i * 64, 64) + 8 * u, 8), :] = zero
            return carry

        lax.fori_loop(0, PAD * stride // 64, clear_edge, 0)

    def clear(i, carry):
        for u in range(32):
            acc[pl.ds(pl.multiple_of(i * 256, 256) + 8 * u, 8), :] = zero
        return carry

    lax.fori_loop(0, acc.shape[0] // 256, clear, 0)

    span = 4096
    for j in range(PIECES):
        shape_copy(j).wait()

        def multiply(s, carry):
            at = pl.multiple_of(j * piece + s * span, span)
            product = jnp.dot(rows, shp[:, pl.ds(at, span)], preferred_element_type=jnp.float32)
            for c in range(span // LANES):
                spot = (PAD + at // LANES + c) * stride
                boxes[pl.ds(spot, count), :] = product[:, c * LANES : (c + 1) * LANES]
            return carry

        lax.fori_loop(0, piece // span, multiply, 0)
    word_copy.wait()

    lane = lax.broadcasted_iota(jnp.int32, (8, LANES), 1)
    pitch = WINDOWS * NY
    owned = words[8 + CHUNKS - 1, 0]

    def out_copy(z, v):
        width = min(LANES, NX - v * LANES)
        slot = lax.rem(z, 2 * DEEP)
        return pltpu.make_async_copy(
            stage.at[slot, v] if width == LANES else tail.at[slot],
            out_ref.at[z, :, pl.ds(v * LANES, width)],
            out_sem.at[slot, v],
        )

    def chunk(c, carry):
        near = words[8 + c, 0]
        total = near + words[8 + c, 1]

        def place(step, carry):
            for u in range(UNROLL):
                item = step * UNROLL + u
                slot = jnp.where(item < near, item, jnp.minimum(owned - near + item, count - 1))
                source = jnp.where(item < total, words[0, slot] + c * (DEEP * 8 * stride), 0)
                base = words[1, slot] + c * (DEEP * pitch)
                turn = words[2, slot]
                part = lax.shift_right_logical(lax.bitwise_and(lane - turn, LANES - 1), 5)
                masks = [part == g for g in range(4)]
                for k in range(DEEP):
                    value = boxes[pl.ds(source + k * 8 * stride, 8, stride=stride), :]
                    value = pltpu.roll(value, turn, 1)
                    for g in range(4):
                        at = pl.ds(base + k * pitch + g, 8, stride=4)
                        acc[at, :] = acc[at, :] + jnp.where(masks[g], value, 0.0)
            return carry

        lax.fori_loop(0, (total + UNROLL - 1) // UNROLL, place, 0)

        def finish(k, carry):
            z = c * DEEP + k

            @pl.when(z >= 2 * DEEP)
            def _():
                for v in range(TILES):
                    out_copy(z - 2 * DEEP, v).wait()

            slot = lax.rem(z, 2 * DEEP)
            base = z * pitch
            for r in range(4):
                x_of = lax.bitwise_and(lane - 32 * r, LANES - 1)
                for i in range(NY // 32):
                    parts = [acc[pl.ds(base + t * NY + r + 32 * i, 8, stride=4), :] for t in range(WINDOWS)]
                    for v in range(TILES):
                        sum_v = None
                        for t in range(WINDOWS):
                            low = max(STEP * t - LANES * v, 0)
                            high = min(STEP * t + LANES - LANES * v, LANES)
                            if low >= min(high, NX - LANES * v):
                                continue
                            value = parts[t]
                            if low > 0:
                                value = jnp.where(x_of >= low, value, 0.0)
                            elif high < LANES and min(high, NX - LANES * v) == high:
                                value = jnp.where(x_of < high, value, 0.0)
                            sum_v = value if sum_v is None else sum_v + value
                        if r:
                            sum_v = pltpu.roll(sum_v, LANES - 32 * r, 1)
                        at = pl.ds(r + 32 * i, 8, stride=4)
                        if (v + 1) * LANES > NX:
                            tail[slot, at, :] = sum_v[:, :TAIL]
                        else:
                            stage[slot, v, at, :] = sum_v
            for v in range(TILES):
                out_copy(z, v).start()
            return carry

        lax.fori_loop(0, DEEP, finish, 0)
        return carry

    lax.fori_loop(0, CHUNKS, chunk, 0)
    for z in range(ZS - 2 * DEEP, ZS):
        for v in range(TILES):
            out_copy(jnp.int32(z), v).wait()


def place_boxes(packed, corners, shapes, slots):
    stride = 2 * slots + 1
    count, columns = shapes.shape
    any_space = pl.BlockSpec(memory_space=pl.ANY)
    vmem = pl.BlockSpec(memory_space=pltpu.VMEM)
    return pl.pallas_call(
        functools.partial(place_kernel, slots, stride),
        out_shape=jax.ShapeDtypeStruct((ZS, NY, NX), jnp.float32),
        in_specs=[vmem, vmem, any_space],
        out_specs=any_space,
        scratch_shapes=[
            pltpu.VMEM((count, columns), jnp.bfloat16),
            pltpu.VMEM(((columns // LANES + 2 * PAD) * stride + 8, LANES), jnp.float32),
            pltpu.VMEM((ZS * WINDOWS * NY, LANES), jnp.float32),
            pltpu.VMEM((2 * DEEP, NX // LANES, NY, LANES), jnp.float32),
            pltpu.VMEM((2 * DEEP, NY, max(TAIL, 1)), jnp.float32),
            pltpu.VMEM((8 + CHUNKS, 2 * slots), jnp.int32),
            pltpu.SMEM((8 + CHUNKS, 2 * slots), jnp.int32),
            pltpu.SemaphoreType.DMA((PIECES,)),
            pltpu.SemaphoreType.DMA,
            pltpu.SemaphoreType.DMA((2 * DEEP, TILES)),
        ],
        compiler_params=pltpu.CompilerParams(vmem_limit_bytes=63 * 1024 * 1024),
    )(packed, corners, shapes)


def share_kernel(bands, slabs, part_ref, out_ref, parts, mine, rows, send_a, recv_a, send_b, recv_b):
    band = lax.axis_index("band")
    slab = lax.axis_index("grid")
    barrier = pltpu.get_barrier_semaphore()
    mesh_id = pl.DeviceIdType.MESH

    def band_peer(d):
        return (lax.rem(band + d, bands), slab)

    def slab_peer(d):
        return (band, lax.rem(slab + d, slabs))

    peers = [band_peer(d) for d in range(1, bands)] + [slab_peer(d) for d in range(1, slabs)]
    for peer in peers:
        pl.semaphore_signal(barrier, inc=1, device_id=peer, device_id_type=mesh_id)
    pl.semaphore_wait(barrier, len(peers))

    copies = []
    for d in range(1, bands):
        copy = pltpu.make_async_remote_copy(
            src_ref=part_ref, dst_ref=parts.at[band], send_sem=send_a.at[d - 1],
            recv_sem=recv_a.at[d - 1], device_id=band_peer(d), device_id_type=mesh_id,
        )
        copy.start()
        copies.append(copy)
    parts[band] = part_ref[...]
    for copy in copies:
        copy.wait()
    total = parts[0]
    for b in range(1, bands):
        total = total + parts[b]
    packed = total.astype(jnp.bfloat16)
    mine[...] = packed
    copies = []
    for d in range(1, slabs):
        copy = pltpu.make_async_remote_copy(
            src_ref=mine, dst_ref=rows.at[slab], send_sem=send_b.at[d - 1],
            recv_sem=recv_b.at[d - 1], device_id=slab_peer(d), device_id_type=mesh_id,
        )
        copy.start()
        copies.append(copy)
    rows[slab] = packed
    for copy in copies:
        copy.wait()
    out_ref[...] = rows[...]


def share(part, bands, slabs):
    count, width = part.shape
    vmem = pl.BlockSpec(memory_space=pltpu.VMEM)
    return pl.pallas_call(
        functools.partial(share_kernel, bands, slabs),
        out_shape=jax.ShapeDtypeStruct((slabs, count, width), jnp.bfloat16),
        in_specs=[vmem],
        out_specs=vmem,
        scratch_shapes=[
            pltpu.VMEM((bands, count, width), jnp.float32),
            pltpu.VMEM((count, width), jnp.bfloat16),
            pltpu.VMEM((slabs, count, width), jnp.bfloat16),
            pltpu.SemaphoreType.DMA((bands - 1,)),
            pltpu.SemaphoreType.DMA((bands - 1,)),
            pltpu.SemaphoreType.DMA((slabs - 1,)),
            pltpu.SemaphoreType.DMA((slabs - 1,)),
        ],
        compiler_params=pltpu.CompilerParams(collective_id=0, has_side_effects=True),
    )(part)


def body(coefficients, occupation, shapes, corners):
    part = occupancy(coefficients, occupation)
    packed = share(part, lax.axis_size("band"), lax.axis_size("grid"))
    packed = packed.reshape(-1, part.shape[1])
    return place_boxes(packed, corners, shapes, 2 * coefficients.shape[0])


def solution(mesh):
    placed = (P("grid", None, "band"), P("band"), P(), P())
    return jax.shard_map(
        body, mesh=mesh, in_specs=placed, out_specs=P("grid", None, None), check_vma=False
    )
```

```python
import functools

import jax
import jax.numpy as jnp
from jax import lax
from jax.experimental import pallas as pl
from jax.experimental.pallas import tpu as pltpu
from jax.sharding import PartitionSpec as P

BOX = 32
ZS = 32
NY = 288
NX = 288
LANES = 128
STEP = LANES - BOX
HALF = LANES // 2


WINDOWS = (NX - BOX) // STEP + 1
TILES = -(-NX // LANES)
TAIL = NX % LANES
DEEP = 4
CHUNKS = ZS // DEEP
PAD = 8 * DEEP
PIECES = 4
UNROLL = 16


def place_kernel(
    slots, stride, packed_ref, corners_ref, shapes_ref, out_ref,
    shp, boxes, acc, stage, tail, table, words, shape_sem, word_sem, out_sem,
):
    slab = lax.axis_index("grid")
    atoms = corners_ref.shape[1]
    columns = shapes_ref.shape[1]
    piece = columns // PIECES
    count = 2 * slots

    def shape_copy(j):
        cols = pl.ds(j * piece, piece)
        return pltpu.make_async_copy(shapes_ref.at[:, cols], shp.at[:, cols], shape_sem.at[j])

    for j in range(PIECES):
        shape_copy(j).start()

    depth = corners_ref[0:1, :]
    owner = lax.shift_right_logical(depth, ZS.bit_length() - 1)
    local = depth - owner * ZS
    own = owner == slab
    below = jnp.logical_and(owner == slab - 1, local > 0)
    index = lax.broadcasted_iota(jnp.int32, (1, atoms), 1)
    key = jnp.where(own, local, jnp.where(below, 2 * ZS - local, 2 * ZS)) * atoms + index
    key = key.astype(jnp.float32)
    slot_rows = []
    for a in range(atoms // LANES):
        mine = key[:, a * LANES : (a + 1) * LANES]
        rank = jnp.zeros((1, LANES), jnp.float32)
        for b in range(atoms // LANES):
            other = jnp.broadcast_to(key[:, b * LANES : (b + 1) * LANES], (LANES, LANES)).T
            rank = rank + jnp.sum((other < mine).astype(jnp.float32), axis=0, keepdims=True)
        slot_rows.append(rank)
    slot_of = jnp.concatenate(slot_rows, axis=1).astype(jnp.int32)
    hot = lax.broadcasted_iota(jnp.int32, (count, atoms), 0) == slot_of
    hot = hot.astype(jnp.float32).astype(jnp.bfloat16)

    slabs, lines, _ = packed_ref.shape
    share = lines * 2 // 3
    firsts, rests = [], []
    for s in range(slabs):
        firsts.append(packed_ref[s, :share, :])
        rests.extend([packed_ref[s, share:, :]] * 2)
    lane = lax.broadcasted_iota(jnp.int32, (atoms, LANES), 1)
    side = lax.rem(lax.broadcasted_iota(jnp.int32, (atoms, LANES), 0), share) >= share // 2
    rest = jnp.concatenate(rests, axis=0).astype(jnp.float32)
    rest = jnp.where(lane == LANES - 1, side.astype(jnp.float32), rest).astype(jnp.bfloat16)
    first = jnp.dot(hot, jnp.concatenate(firsts, axis=0), preferred_element_type=jnp.float32)
    rest = jnp.dot(hot, rest, preferred_element_type=jnp.float32)
    rest = jnp.where(rest[:, LANES - 1 :] > 0.5, pltpu.roll(rest, HALF, 1), rest)
    pairs = shapes_ref.shape[0]
    rows = jnp.concatenate([first, rest[:, : pairs - LANES]], axis=1).astype(jnp.bfloat16)

    start = jnp.where(own, -local, ZS - local)
    line = lax.broadcasted_iota(jnp.int32, (8, atoms), 0)
    traits = jnp.where(line == 0, corners_ref[1:2, :], jnp.where(line == 1, corners_ref[2:3, :], start))
    traits = traits.astype(jnp.float32).astype(jnp.bfloat16)
    traits = lax.dot_general(traits, hot, (((1,), (1,)), ((), ())), preferred_element_type=jnp.float32)
    traits = traits.astype(jnp.int32)
    row, column, start = traits[0:1, :], traits[1:2, :], traits[2:3, :]
    window = jnp.zeros_like(column)
    for t in range(1, WINDOWS):
        window = window + (column >= t * STEP).astype(jnp.int32)
    source = (PAD + start * 8) * stride + lax.broadcasted_iota(jnp.int32, (1, count), 1)
    target = window * NY + row
    turn = lax.bitwise_and(column + 32 * row, LANES - 1)
    line = lax.broadcasted_iota(jnp.int32, (8, count), 0)
    table[0:8, :] = jnp.where(line == 0, source, jnp.where(line == 1, target, turn))
    bound = lax.broadcasted_iota(jnp.int32, (CHUNKS, atoms), 0) * DEEP
    near = jnp.sum(jnp.where(jnp.logical_and(own, local < bound + DEEP), 1.0, 0.0), axis=1, keepdims=True)
    far = jnp.sum(jnp.where(jnp.logical_and(below, local > bound), 1.0, 0.0), axis=1, keepdims=True)
    side = lax.broadcasted_iota(jnp.int32, (CHUNKS, count), 1)
    table[8 : 8 + CHUNKS, :] = jnp.where(side == 0, near, far).astype(jnp.int32)
    word_copy = pltpu.make_async_copy(table, words, word_sem)
    word_copy.start()

    zero = jnp.zeros((8, LANES), jnp.float32)
    for edge in (0, PAD + columns // LANES):
        def clear_edge(i, carry):
            for u in range(8):
                boxes[pl.ds(edge * stride + pl.multiple_of(i * 64, 64) + 8 * u, 8), :] = zero
            return carry

        lax.fori_loop(0, PAD * stride // 64, clear_edge, 0)

    def clear(i, carry):
        for u in range(32):
            acc[pl.ds(pl.multiple_of(i * 256, 256) + 8 * u, 8), :] = zero
        return carry

    lax.fori_loop(0, acc.shape[0] // 256, clear, 0)

    span = 4096
    for j in range(PIECES):
        shape_copy(j).wait()

        def multiply(s, carry):
            at = pl.multiple_of(j * piece + s * span, span)
            product = jnp.dot(rows, shp[:, pl.ds(at, span)], preferred_element_type=jnp.float32)
            for c in range(span // LANES):
                spot = (PAD + at // LANES + c) * stride
                boxes[pl.ds(spot, count), :] = product[:, c * LANES : (c + 1) * LANES]
            return carry

        lax.fori_loop(0, piece // span, multiply, 0)
    word_copy.wait()

    lane = lax.broadcasted_iota(jnp.int32, (8, LANES), 1)
    pitch = WINDOWS * NY
    owned = words[8 + CHUNKS - 1, 0]

    def out_copy(z, v):
        width = min(LANES, NX - v * LANES)
        slot = lax.rem(z, 2 * DEEP)
        return pltpu.make_async_copy(
            stage.at[slot, v] if width == LANES else tail.at[slot],
            out_ref.at[z, :, pl.ds(v * LANES, width)],
            out_sem.at[slot, v],
        )

    def chunk(c, carry):
        near = words[8 + c, 0]
        total = near + words[8 + c, 1]

        def place(step, carry):
            for u in range(UNROLL):
                item = step * UNROLL + u
                slot = jnp.where(item < near, item, jnp.minimum(owned - near + item, count - 1))
                source = jnp.where(item < total, words[0, slot] + c * (DEEP * 8 * stride), 0)
                base = words[1, slot] + c * (DEEP * pitch)
                turn = words[2, slot]
                part = lax.shift_right_logical(lax.bitwise_and(lane - turn, LANES - 1), 5)
                masks = [part == g for g in range(4)]
                for k in range(DEEP):
                    value = boxes[pl.ds(source + k * 8 * stride, 8, stride=stride), :]
                    value = pltpu.roll(value, turn, 1)
                    for g in range(4):
                        at = pl.ds(base + k * pitch + g, 8, stride=4)
                        acc[at, :] = acc[at, :] + jnp.where(masks[g], value, 0.0)
            return carry

        lax.fori_loop(0, (total + UNROLL - 1) // UNROLL, place, 0)

        def finish(k, carry):
            z = c * DEEP + k

            @pl.when(z >= 2 * DEEP)
            def _():
                for v in range(TILES):
                    out_copy(z - 2 * DEEP, v).wait()

            slot = lax.rem(z, 2 * DEEP)
            base = z * pitch
            for r in range(4):
                x_of = lax.bitwise_and(lane - 32 * r, LANES - 1)
                for i in range(NY // 32):
                    parts = [acc[pl.ds(base + t * NY + r + 32 * i, 8, stride=4), :] for t in range(WINDOWS)]
                    for v in range(TILES):
                        sum_v = None
                        for t in range(WINDOWS):
                            low = max(STEP * t - LANES * v, 0)
                            high = min(STEP * t + LANES - LANES * v, LANES)
                            if low >= min(high, NX - LANES * v):
                                continue
                            value = parts[t]
                            if low > 0:
                                value = jnp.where(x_of >= low, value, 0.0)
                            elif high < LANES and min(high, NX - LANES * v) == high:
                                value = jnp.where(x_of < high, value, 0.0)
                            sum_v = value if sum_v is None else sum_v + value
                        if r:
                            sum_v = pltpu.roll(sum_v, LANES - 32 * r, 1)
                        at = pl.ds(r + 32 * i, 8, stride=4)
                        if (v + 1) * LANES > NX:
                            tail[slot, at, :] = sum_v[:, :TAIL]
                        else:
                            stage[slot, v, at, :] = sum_v
            for v in range(TILES):
                out_copy(z, v).start()
            return carry

        lax.fori_loop(0, DEEP, finish, 0)
        return carry

    lax.fori_loop(0, CHUNKS, chunk, 0)
    for z in range(ZS - 2 * DEEP, ZS):
        for v in range(TILES):
            out_copy(jnp.int32(z), v).wait()


def place_boxes(packed, corners, shapes, slots):
    stride = 2 * slots + 1
    count, columns = shapes.shape
    any_space = pl.BlockSpec(memory_space=pl.ANY)
    vmem = pl.BlockSpec(memory_space=pltpu.VMEM)
    return pl.pallas_call(
        functools.partial(place_kernel, slots, stride),
        out_shape=jax.ShapeDtypeStruct((ZS, NY, NX), jnp.float32),
        in_specs=[vmem, vmem, any_space],
        out_specs=any_space,
        scratch_shapes=[
            pltpu.VMEM((count, columns), jnp.bfloat16),
            pltpu.VMEM(((columns // LANES + 2 * PAD) * stride + 8, LANES), jnp.float32),
            pltpu.VMEM((ZS * WINDOWS * NY, LANES), jnp.float32),
            pltpu.VMEM((2 * DEEP, NX // LANES, NY, LANES), jnp.float32),
            pltpu.VMEM((2 * DEEP, NY, max(TAIL, 1)), jnp.float32),
            pltpu.VMEM((8 + CHUNKS, 2 * slots), jnp.int32),
            pltpu.SMEM((8 + CHUNKS, 2 * slots), jnp.int32),
            pltpu.SemaphoreType.DMA((PIECES,)),
            pltpu.SemaphoreType.DMA,
            pltpu.SemaphoreType.DMA((2 * DEEP, TILES)),
        ],
        compiler_params=pltpu.CompilerParams(vmem_limit_bytes=63 * 1024 * 1024),
    )(packed, corners, shapes)


def share_kernel(
    bands, slabs, coef_ref, occupation_ref, out_ref,
    raw, level, plain, heavy, part, parts, mine, rows, load_sem, send_a, recv_a, send_b, recv_b,
):
    band = lax.axis_index("band")
    slab = lax.axis_index("grid")
    barrier = pltpu.get_barrier_semaphore()
    mesh_id = pl.DeviceIdType.MESH

    def band_peer(d):
        return (lax.rem(band + d, bands), slab)

    def slab_peer(d):
        return (band, lax.rem(slab + d, slabs))

    peers = [band_peer(d) for d in range(1, bands)] + [slab_peer(d) for d in range(1, slabs)]
    for peer in peers:
        pl.semaphore_signal(barrier, inc=1, device_id=peer, device_id_type=mesh_id)
    loads = [
        pltpu.make_async_copy(occupation_ref, level, load_sem.at[0]),
        pltpu.make_async_copy(coef_ref, raw, load_sem.at[1]),
    ]
    for load in loads:
        load.start()
    for load in loads:
        load.wait()
    weight = level[...].astype(jnp.float32) * 0.5

    projectors, atoms, depth = raw.shape
    half = atoms // 2
    for i in range(projectors):
        value = raw[i].astype(jnp.float32)
        plain[i] = value
        heavy[i] = value * weight
    lane = lax.broadcasted_iota(jnp.int32, (1, LANES), 1)
    main = jnp.zeros((atoms, LANES), jnp.float32)
    rest = jnp.zeros((half, LANES), jnp.float32)
    pair = 0
    for i in range(projectors):
        left = plain[i]
        for j in range(i, projectors):
            product = left * heavy[j]
            total = product[:, :LANES]
            for v in range(1, depth // LANES):
                total = total + product[:, v * LANES : (v + 1) * LANES]
            total = jnp.sum(total, axis=1, keepdims=True)
            if i == j:
                total = total * 0.5
            if pair < LANES:
                main = jnp.where(lane == pair, total, main)
            else:
                rest = jnp.where(lane == pair - LANES, total[:half], rest)
                rest = jnp.where(lane == pair - HALF, total[half:], rest)
            pair = pair + 1
    part[:atoms, :] = main
    part[atoms:, :] = rest
    pl.semaphore_wait(barrier, len(peers))

    copies = []
    for d in range(1, bands):
        copy = pltpu.make_async_remote_copy(
            src_ref=part, dst_ref=parts.at[band], send_sem=send_a.at[d - 1],
            recv_sem=recv_a.at[d - 1], device_id=band_peer(d), device_id_type=mesh_id,
        )
        copy.start()
        copies.append(copy)
    parts[band] = part[...]
    for copy in copies:
        copy.wait()
    total = parts[0]
    for b in range(1, bands):
        total = total + parts[b]
    packed = total.astype(jnp.bfloat16)
    mine[...] = packed
    copies = []
    for d in range(1, slabs):
        copy = pltpu.make_async_remote_copy(
            src_ref=mine, dst_ref=rows.at[slab], send_sem=send_b.at[d - 1],
            recv_sem=recv_b.at[d - 1], device_id=slab_peer(d), device_id_type=mesh_id,
        )
        copy.start()
        copies.append(copy)
    rows[slab] = packed
    for copy in copies:
        copy.wait()
    out_ref[...] = rows[...]


def share(coefficients, occupation, bands, slabs):
    atoms, projectors, depth = coefficients.shape
    lines = atoms + atoms // 2
    f32 = jnp.float32
    return pl.pallas_call(
        functools.partial(share_kernel, bands, slabs),
        out_shape=pltpu.VMEM((slabs, lines, LANES), jnp.bfloat16),
        in_specs=[pl.BlockSpec(memory_space=pltpu.HBM)] * 2,
        out_specs=pl.BlockSpec(memory_space=pltpu.VMEM),
        scratch_shapes=[
            pltpu.VMEM((projectors, atoms, depth), jnp.bfloat16),
            pltpu.VMEM((1, depth), jnp.int32),
            pltpu.VMEM((projectors, atoms, depth), f32),
            pltpu.VMEM((projectors, atoms, depth), f32),
            pltpu.VMEM((lines, LANES), f32),
            pltpu.VMEM((bands, lines, LANES), f32),
            pltpu.VMEM((lines, LANES), jnp.bfloat16),
            pltpu.VMEM((slabs, lines, LANES), jnp.bfloat16),
            pltpu.SemaphoreType.DMA((2,)),
            pltpu.SemaphoreType.DMA((bands - 1,)),
            pltpu.SemaphoreType.DMA((bands - 1,)),
            pltpu.SemaphoreType.DMA((slabs - 1,)),
            pltpu.SemaphoreType.DMA((slabs - 1,)),
        ],
        compiler_params=pltpu.CompilerParams(
            collective_id=0, has_side_effects=True, vmem_limit_bytes=8 * 1024 * 1024
        ),
    )(
        pltpu.with_memory_space_constraint(jnp.transpose(coefficients, (1, 0, 2)), pltpu.HBM),
        pltpu.with_memory_space_constraint(occupation.reshape(1, depth), pltpu.HBM),
    )


def body(coefficients, occupation, shapes, corners):
    packed = share(coefficients, occupation, lax.axis_size("band"), lax.axis_size("grid"))
    packed = pltpu.with_memory_space_constraint(packed, pltpu.VMEM)
    return place_boxes(packed, corners, shapes, 2 * coefficients.shape[0])


def solution(mesh):
    placed = (P("grid", None, "band"), P("band"), P(), P())
    return jax.shard_map(
        body, mesh=mesh, in_specs=placed, out_specs=P("grid", None, None), check_vma=False
    )
```

```python
import functools

import jax
import jax.numpy as jnp
from jax import lax
from jax.experimental import pallas as pl
from jax.experimental.pallas import tpu as pltpu
from jax.sharding import PartitionSpec as P

BOX = 32
ZS = 32
NY = 288
NX = 288
LANES = 128
STEP = LANES - BOX
HALF = LANES // 2


WINDOWS = (NX - BOX) // STEP + 1
TILES = -(-NX // LANES)
TAIL = NX % LANES
DEEP = 4
CHUNKS = ZS // DEEP
PAD = 8 * DEEP
PIECES = 4
UNROLL = 16


def place_kernel(
    slots, stride, packed_ref, corners_ref, shapes_ref, out_ref,
    shp, boxes, *refs,
):
    accs, refs = refs[:DEEP], refs[DEEP:]
    stage, tail, table, counts, sources, targets, turns, sizes, shape_sem, word_sem, out_sem = refs
    slab = lax.axis_index("grid")
    atoms = corners_ref.shape[1]
    columns = shapes_ref.shape[1]
    piece = columns // PIECES
    count = 2 * slots

    def shape_copy(j):
        cols = pl.ds(j * piece, piece)
        return pltpu.make_async_copy(shapes_ref.at[:, cols], shp.at[:, cols], shape_sem.at[j])

    for j in range(PIECES):
        shape_copy(j).start()

    depth = corners_ref[0:1, :]
    owner = lax.shift_right_logical(depth, ZS.bit_length() - 1)
    local = depth - owner * ZS
    own = owner == slab
    below = jnp.logical_and(owner == slab - 1, local > 0)
    index = lax.broadcasted_iota(jnp.int32, (1, atoms), 1)
    key = jnp.where(own, local, jnp.where(below, ZS + 1 + local, ZS)) * atoms + index
    key = key.astype(jnp.float32)
    slot_rows = []
    for a in range(atoms // LANES):
        mine = key[:, a * LANES : (a + 1) * LANES]
        rank = jnp.zeros((1, LANES), jnp.float32)
        for b in range(atoms // LANES):
            other = jnp.broadcast_to(key[:, b * LANES : (b + 1) * LANES], (LANES, LANES)).T
            rank = rank + jnp.sum((other < mine).astype(jnp.float32), axis=0, keepdims=True)
        slot_rows.append(rank)
    slot_of = jnp.concatenate(slot_rows, axis=1).astype(jnp.int32)
    slot_of = jnp.where(own, slot_of, jnp.where(below, slot_of + (count - atoms), -1))
    hot = lax.broadcasted_iota(jnp.int32, (count, atoms), 0) == slot_of
    hot = hot.astype(jnp.float32).astype(jnp.bfloat16)

    slabs, lines, _ = packed_ref.shape
    share = lines * 2 // 3
    firsts, rests = [], []
    for s in range(slabs):
        firsts.append(packed_ref[s, :share, :])
        rests.extend([packed_ref[s, share:, :]] * 2)
    lane = lax.broadcasted_iota(jnp.int32, (atoms, LANES), 1)
    side = lax.rem(lax.broadcasted_iota(jnp.int32, (atoms, LANES), 0), share) >= share // 2
    rest = jnp.concatenate(rests, axis=0).astype(jnp.float32)
    rest = jnp.where(lane == LANES - 1, side.astype(jnp.float32), rest).astype(jnp.bfloat16)
    first = jnp.dot(hot, jnp.concatenate(firsts, axis=0), preferred_element_type=jnp.float32)
    rest = jnp.dot(hot, rest, preferred_element_type=jnp.float32)
    rest = jnp.where(rest[:, LANES - 1 :] > 0.5, pltpu.roll(rest, HALF, 1), rest)
    pairs = shapes_ref.shape[0]
    rows = jnp.concatenate([first, rest[:, : pairs - LANES]], axis=1).astype(jnp.bfloat16)

    start = jnp.where(own, -local, ZS - local)
    line = lax.broadcasted_iota(jnp.int32, (8, atoms), 0)
    traits = jnp.where(line == 0, corners_ref[1:2, :], jnp.where(line == 1, corners_ref[2:3, :], start))
    traits = traits.astype(jnp.float32).astype(jnp.bfloat16)
    traits = lax.dot_general(traits, hot, (((1,), (1,)), ((), ())), preferred_element_type=jnp.float32)
    traits = traits.astype(jnp.int32)
    row, column, start = traits[0:1, :], traits[1:2, :], traits[2:3, :]
    window = jnp.zeros_like(column)
    for t in range(1, WINDOWS):
        window = window + (column >= t * STEP).astype(jnp.int32)
    source = (PAD + start * 8) * stride + lax.broadcasted_iota(jnp.int32, (1, count), 1)
    target = window * NY + row
    turn = lax.bitwise_and(column + 32 * row, LANES - 1)
    for at, value in enumerate((source, target, turn)):
        table[at : at + 1, :] = value
    bound = lax.broadcasted_iota(jnp.int32, (CHUNKS, atoms), 0) * DEEP
    near = jnp.sum(jnp.where(jnp.logical_and(own, local < bound + DEEP), 1.0, 0.0), axis=1, keepdims=True)
    far = jnp.sum(jnp.where(jnp.logical_and(below, local > bound), 1.0, 0.0), axis=1, keepdims=True)
    side = lax.broadcasted_iota(jnp.int32, (CHUNKS, LANES), 1)
    counts[...] = jnp.where(side == 0, near, far).astype(jnp.int32)
    word_copies = [
        pltpu.make_async_copy(table.at[0], sources, word_sem.at[0]),
        pltpu.make_async_copy(table.at[1], targets, word_sem.at[1]),
        pltpu.make_async_copy(table.at[2], turns, word_sem.at[2]),
        pltpu.make_async_copy(counts, sizes, word_sem.at[3]),
    ]
    for copy in word_copies:
        copy.start()

    zero = jnp.zeros((8, LANES), jnp.float32)
    for edge in (0, PAD + columns // LANES):
        def clear_edge(i, carry):
            for u in range(8):
                boxes[pl.ds(edge * stride + pl.multiple_of(i * 64, 64) + 8 * u, 8), :] = zero
            return carry

        lax.fori_loop(0, PAD * stride // 64, clear_edge, 0)

    def clear(i, carry):
        for acc in accs:
            for u in range(8):
                acc[pl.ds(pl.multiple_of(i * 64, 64) + 8 * u, 8), :] = zero
        return carry

    lax.fori_loop(0, accs[0].shape[0] // 64, clear, 0)

    span = 4096
    for j in range(PIECES):
        shape_copy(j).wait()

        def multiply(s, carry):
            at = pl.multiple_of(j * piece + s * span, span)
            product = jnp.dot(rows, shp[:, pl.ds(at, span)], preferred_element_type=jnp.float32)
            for c in range(span // LANES):
                spot = (PAD + at // LANES + c) * stride
                boxes[pl.ds(spot, count), :] = product[:, c * LANES : (c + 1) * LANES]
            return carry

        lax.fori_loop(0, piece // span, multiply, 0)
    for copy in word_copies:
        copy.wait()

    lane = lax.broadcasted_iota(jnp.int32, (8, LANES), 1)
    pitch = WINDOWS * NY

    def out_copy(c, k, v):
        width = min(LANES, NX - v * LANES)
        slot = lax.rem(c, 2) * DEEP + k
        return pltpu.make_async_copy(
            stage.at[slot, v] if width == LANES else tail.at[slot],
            out_ref.at[c * DEEP + k, :, pl.ds(v * LANES, width)],
            out_sem.at[slot, v],
        )

    def chunk(c, carry):
        far = sizes[c, 1]
        total = sizes[c, 0] + far

        def place(step, carry):
            for u in range(UNROLL):
                item = step * UNROLL + u
                slot = lax.bitwise_and(item - far, count - 1)
                source = jnp.where(item < total, sources[slot] + c * (DEEP * 8 * stride), 0)
                base = targets[slot] + c * pitch
                turn = turns[slot]
                part = lax.shift_right_logical(lax.bitwise_and(lane - turn, LANES - 1), 5)
                masks = [part == g for g in range(4)]
                for k in range(DEEP):
                    value = boxes[pl.ds(source + k * 8 * stride, 8, stride=stride), :]
                    value = pltpu.roll(value, turn, 1)
                    for g in range(4):
                        at = pl.ds(base + g, 8, stride=4)
                        accs[k][at, :] = accs[k][at, :] + jnp.where(masks[g], value, 0.0)
            return carry

        lax.fori_loop(0, (total + UNROLL - 1) // UNROLL, place, 0)

        @pl.when(c >= 2)
        def _():
            for k in range(DEEP):
                for v in range(TILES):
                    out_copy(c - 2, k, v).wait()

        bank = lax.rem(c, 2)
        for k in range(DEEP):
            slot = bank * DEEP + k
            for r in range(4):
                x_of = lax.bitwise_and(lane - 32 * r, LANES - 1)
                for i in range(NY // 32):
                    first = c * pitch + r + 32 * i
                    parts = [accs[k][pl.ds(first + t * NY, 8, stride=4), :] for t in range(WINDOWS)]
                    for v in range(TILES):
                        sum_v = None
                        for t in range(WINDOWS):
                            low = max(STEP * t - LANES * v, 0)
                            high = min(STEP * t + LANES - LANES * v, LANES)
                            if low >= min(high, NX - LANES * v):
                                continue
                            value = parts[t]
                            if low > 0:
                                value = jnp.where(x_of >= low, value, 0.0)
                            elif high < LANES and min(high, NX - LANES * v) == high:
                                value = jnp.where(x_of < high, value, 0.0)
                            sum_v = value if sum_v is None else sum_v + value
                        if r:
                            sum_v = pltpu.roll(sum_v, LANES - 32 * r, 1)
                        at = pl.ds(r + 32 * i, 8, stride=4)
                        if (v + 1) * LANES > NX:
                            tail[slot, at, :] = sum_v[:, :TAIL]
                        else:
                            stage[slot, v, at, :] = sum_v
            for v in range(TILES):
                out_copy(c, k, v).start()
        return carry

    lax.fori_loop(0, CHUNKS, chunk, 0)
    for c in (CHUNKS - 2, CHUNKS - 1):
        for k in range(DEEP):
            for v in range(TILES):
                out_copy(jnp.int32(c), k, v).wait()


def place_boxes(packed, corners, shapes, slots):
    stride = 2 * slots + 1
    count, columns = shapes.shape
    any_space = pl.BlockSpec(memory_space=pl.ANY)
    vmem = pl.BlockSpec(memory_space=pltpu.VMEM)
    return pl.pallas_call(
        functools.partial(place_kernel, slots, stride),
        out_shape=jax.ShapeDtypeStruct((ZS, NY, NX), jnp.float32),
        in_specs=[vmem, vmem, any_space],
        out_specs=any_space,
        scratch_shapes=[
            pltpu.VMEM((count, columns), jnp.bfloat16),
            pltpu.VMEM(((columns // LANES + 2 * PAD) * stride + 8, LANES), jnp.float32),
            *[pltpu.VMEM((CHUNKS * WINDOWS * NY, LANES), jnp.float32)] * DEEP,
            pltpu.VMEM((2 * DEEP, NX // LANES, NY, LANES), jnp.float32),
            pltpu.VMEM((2 * DEEP, NY, max(TAIL, 1)), jnp.float32),
            pltpu.VMEM((8, 2 * slots), jnp.int32),
            pltpu.VMEM((CHUNKS, LANES), jnp.int32),
            *[pltpu.SMEM((2 * slots,), jnp.int32)] * 3,
            pltpu.SMEM((CHUNKS, LANES), jnp.int32),
            pltpu.SemaphoreType.DMA((PIECES,)),
            pltpu.SemaphoreType.DMA((4,)),
            pltpu.SemaphoreType.DMA((2 * DEEP, TILES)),
        ],
        compiler_params=pltpu.CompilerParams(vmem_limit_bytes=63 * 1024 * 1024),
    )(packed, corners, shapes)


def share_kernel(
    bands, slabs, coef_ref, occupation_ref, out_ref,
    raw, level, plain, heavy, part, parts, mine, rows, load_sem, send_a, recv_a, send_b, recv_b,
):
    band = lax.axis_index("band")
    slab = lax.axis_index("grid")
    barrier = pltpu.get_barrier_semaphore()
    mesh_id = pl.DeviceIdType.MESH

    def band_peer(d):
        return (lax.rem(band + d, bands), slab)

    def slab_peer(d):
        return (band, lax.rem(slab + d, slabs))

    peers = [band_peer(d) for d in range(1, bands)] + [slab_peer(d) for d in range(1, slabs)]
    for peer in peers:
        pl.semaphore_signal(barrier, inc=1, device_id=peer, device_id_type=mesh_id)
    loads = [
        pltpu.make_async_copy(occupation_ref, level, load_sem.at[0]),
        pltpu.make_async_copy(coef_ref, raw, load_sem.at[1]),
    ]
    for load in loads:
        load.start()
    for load in loads:
        load.wait()
    weight = level[...].astype(jnp.float32) * 0.5

    projectors, atoms, depth = raw.shape
    half = atoms // 2
    for i in range(projectors):
        value = raw[i].astype(jnp.float32)
        plain[i] = value
        heavy[i] = value * weight
    lane = lax.broadcasted_iota(jnp.int32, (1, LANES), 1)
    main = jnp.zeros((atoms, LANES), jnp.float32)
    rest = jnp.zeros((half, LANES), jnp.float32)
    pair = 0
    for i in range(projectors):
        left = plain[i]
        for j in range(i, projectors):
            product = left * heavy[j]
            total = product[:, :LANES]
            for v in range(1, depth // LANES):
                total = total + product[:, v * LANES : (v + 1) * LANES]
            total = jnp.sum(total, axis=1, keepdims=True)
            if i == j:
                total = total * 0.5
            if pair < LANES:
                main = jnp.where(lane == pair, total, main)
            else:
                rest = jnp.where(lane == pair - LANES, total[:half], rest)
                rest = jnp.where(lane == pair - HALF, total[half:], rest)
            pair = pair + 1
    part[:atoms, :] = main
    part[atoms:, :] = rest
    pl.semaphore_wait(barrier, len(peers))

    copies = []
    for d in range(1, bands):
        copy = pltpu.make_async_remote_copy(
            src_ref=part, dst_ref=parts.at[band], send_sem=send_a.at[d - 1],
            recv_sem=recv_a.at[d - 1], device_id=band_peer(d), device_id_type=mesh_id,
        )
        copy.start()
        copies.append(copy)
    parts[band] = part[...]
    for copy in copies:
        copy.wait()
    total = parts[0]
    for b in range(1, bands):
        total = total + parts[b]
    packed = total.astype(jnp.bfloat16)
    mine[...] = packed
    copies = []
    for d in range(1, slabs):
        copy = pltpu.make_async_remote_copy(
            src_ref=mine, dst_ref=rows.at[slab], send_sem=send_b.at[d - 1],
            recv_sem=recv_b.at[d - 1], device_id=slab_peer(d), device_id_type=mesh_id,
        )
        copy.start()
        copies.append(copy)
    rows[slab] = packed
    for copy in copies:
        copy.wait()
    out_ref[...] = rows[...]


def share(coefficients, occupation, bands, slabs):
    atoms, projectors, depth = coefficients.shape
    lines = atoms + atoms // 2
    f32 = jnp.float32
    return pl.pallas_call(
        functools.partial(share_kernel, bands, slabs),
        out_shape=pltpu.VMEM((slabs, lines, LANES), jnp.bfloat16),
        in_specs=[pl.BlockSpec(memory_space=pltpu.HBM)] * 2,
        out_specs=pl.BlockSpec(memory_space=pltpu.VMEM),
        scratch_shapes=[
            pltpu.VMEM((projectors, atoms, depth), jnp.bfloat16),
            pltpu.VMEM((1, depth), jnp.int32),
            pltpu.VMEM((projectors, atoms, depth), f32),
            pltpu.VMEM((projectors, atoms, depth), f32),
            pltpu.VMEM((lines, LANES), f32),
            pltpu.VMEM((bands, lines, LANES), f32),
            pltpu.VMEM((lines, LANES), jnp.bfloat16),
            pltpu.VMEM((slabs, lines, LANES), jnp.bfloat16),
            pltpu.SemaphoreType.DMA((2,)),
            pltpu.SemaphoreType.DMA((bands - 1,)),
            pltpu.SemaphoreType.DMA((bands - 1,)),
            pltpu.SemaphoreType.DMA((slabs - 1,)),
            pltpu.SemaphoreType.DMA((slabs - 1,)),
        ],
        compiler_params=pltpu.CompilerParams(
            collective_id=0, has_side_effects=True, vmem_limit_bytes=8 * 1024 * 1024
        ),
    )(
        pltpu.with_memory_space_constraint(jnp.transpose(coefficients, (1, 0, 2)), pltpu.HBM),
        pltpu.with_memory_space_constraint(occupation.reshape(1, depth), pltpu.HBM),
    )


def body(coefficients, occupation, shapes, corners):
    packed = share(coefficients, occupation, lax.axis_size("band"), lax.axis_size("grid"))
    packed = pltpu.with_memory_space_constraint(packed, pltpu.VMEM)
    return place_boxes(packed, corners, shapes, 2 * coefficients.shape[0])


def solution(mesh):
    placed = (P("grid", None, "band"), P("band"), P(), P())
    return jax.shard_map(
        body, mesh=mesh, in_specs=placed, out_specs=P("grid", None, None), check_vma=False
    )
```

```python
import functools

import jax
import jax.numpy as jnp
from jax import lax
from jax.experimental import pallas as pl
from jax.experimental.pallas import tpu as pltpu
from jax.sharding import PartitionSpec as P

BOX = 32
ZS = 32
NY = 288
NX = 288
LANES = 128
STEP = LANES - BOX
HALF = LANES // 2


WINDOWS = (NX - BOX) // STEP + 1
TILES = -(-NX // LANES)
TAIL = NX % LANES
DEEP = 4
CHUNKS = ZS // DEEP
PAD = 8 * DEEP
UNROLL = 16
CARRY = 8


def plan_slots(slab, corners_ref, count, stride, hot_ref, table_ref, counts_ref):
    atoms = corners_ref.shape[1]

    depth = corners_ref[0:1, :]
    owner = lax.shift_right_logical(depth, ZS.bit_length() - 1)
    local = depth - owner * ZS
    own = owner == slab
    below = jnp.logical_and(owner == slab - 1, local > 0)
    index = lax.broadcasted_iota(jnp.int32, (1, atoms), 1)
    key = jnp.where(own, local, jnp.where(below, ZS + 1 + local, ZS)) * atoms + index
    key = key.astype(jnp.float32)
    slot_rows = []
    for a in range(atoms // LANES):
        mine = key[:, a * LANES : (a + 1) * LANES]
        rank = jnp.zeros((1, LANES), jnp.float32)
        for b in range(atoms // LANES):
            other = jnp.broadcast_to(key[:, b * LANES : (b + 1) * LANES], (LANES, LANES)).T
            rank = rank + jnp.sum((other < mine).astype(jnp.float32), axis=0, keepdims=True)
        slot_rows.append(rank)
    slot_of = jnp.concatenate(slot_rows, axis=1).astype(jnp.int32)
    slot_of = jnp.where(own, slot_of, jnp.where(below, slot_of + (count - atoms), -1))
    hot = lax.broadcasted_iota(jnp.int32, (count, atoms), 0) == slot_of
    hot = hot.astype(jnp.float32).astype(jnp.bfloat16)
    hot_ref[...] = hot
    start = jnp.where(own, -local, ZS - local)
    line = lax.broadcasted_iota(jnp.int32, (8, atoms), 0)
    traits = jnp.where(line == 0, corners_ref[1:2, :], jnp.where(line == 1, corners_ref[2:3, :], start))
    traits = traits.astype(jnp.float32).astype(jnp.bfloat16)
    traits = lax.dot_general(traits, hot, (((1,), (1,)), ((), ())), preferred_element_type=jnp.float32)
    traits = traits.astype(jnp.int32)
    row, column, start = traits[0:1, :], traits[1:2, :], traits[2:3, :]
    window = jnp.zeros_like(column)
    for t in range(1, WINDOWS):
        window = window + (column >= t * STEP).astype(jnp.int32)
    source = (PAD + start * 8) * stride + lax.broadcasted_iota(jnp.int32, (1, count), 1)
    target = window * NY + row
    turn = lax.bitwise_and(column + 32 * row, LANES - 1)
    for at, value in enumerate((source, target, turn)):
        table_ref[at : at + 1, :] = value
    bound = lax.broadcasted_iota(jnp.int32, (CHUNKS, atoms), 0) * DEEP
    near = jnp.sum(jnp.where(jnp.logical_and(own, local < bound + DEEP), 1.0, 0.0), axis=1, keepdims=True)
    far = jnp.sum(jnp.where(jnp.logical_and(below, local > bound), 1.0, 0.0), axis=1, keepdims=True)
    side = lax.broadcasted_iota(jnp.int32, (CHUNKS, LANES), 1)
    counts_ref[...] = jnp.where(side == 0, near, far).astype(jnp.int32)


def place_kernel(
    slots, stride, packed_ref, hot_ref, table_ref, counts_ref, shapes_ref, *refs,
):
    out_ref = refs[DEEP]
    accs = refs[DEEP + 1 : 2 * DEEP + 1]
    boxes, stage, tail, sources, targets, turns, sizes, word_sem, out_sem = refs[2 * DEEP + 1 :]
    columns = shapes_ref.shape[1]
    count = 2 * slots
    atoms = hot_ref.shape[1]
    hot = hot_ref[...]
    word_copies = [
        pltpu.make_async_copy(table_ref.at[0], sources, word_sem.at[0]),
        pltpu.make_async_copy(table_ref.at[1], targets, word_sem.at[1]),
        pltpu.make_async_copy(table_ref.at[2], turns, word_sem.at[2]),
        pltpu.make_async_copy(counts_ref, sizes, word_sem.at[3]),
    ]
    for copy in word_copies:
        copy.start()

    slabs, lines, _ = packed_ref.shape
    share = lines * 2 // 3
    firsts, rests = [], []
    for s in range(slabs):
        firsts.append(packed_ref[s, :share, :])
        rests.extend([packed_ref[s, share:, :]] * 2)
    lane = lax.broadcasted_iota(jnp.int32, (atoms, LANES), 1)
    side = lax.rem(lax.broadcasted_iota(jnp.int32, (atoms, LANES), 0), share) >= share // 2
    rest = jnp.concatenate(rests, axis=0).astype(jnp.float32)
    rest = jnp.where(lane == LANES - 1, side.astype(jnp.float32), rest).astype(jnp.bfloat16)
    first = jnp.dot(hot, jnp.concatenate(firsts, axis=0), preferred_element_type=jnp.float32)
    rest = jnp.dot(hot, rest, preferred_element_type=jnp.float32)
    rest = jnp.where(rest[:, LANES - 1 :] > 0.5, pltpu.roll(rest, HALF, 1), rest)
    pairs = shapes_ref.shape[0]
    rows = jnp.concatenate([first, rest[:, : pairs - LANES]], axis=1).astype(jnp.bfloat16)

    span = 4096
    strip = -(-PAD * stride * span // (8 * columns)) * 8
    zero = jnp.zeros((8, LANES), jnp.float32)

    def multiply(s, carry):
        at = pl.multiple_of(s * span, span)
        product = jnp.dot(rows, shapes_ref[:, pl.ds(at, span)], preferred_element_type=jnp.float32)
        for c in range(span // LANES):
            spot = (PAD + at // LANES + c) * stride
            boxes[pl.ds(spot, count), :] = product[:, c * LANES : (c + 1) * LANES]
        edge = jnp.minimum(s * strip, PAD * stride - strip)
        for u in range(strip // 8):
            boxes[pl.ds(edge + 8 * u, 8), :] = zero
            boxes[pl.ds(edge + (PAD + columns // LANES) * stride + 8 * u, 8), :] = zero
        return carry

    lax.fori_loop(0, columns // span, multiply, 0)
    for copy in word_copies:
        copy.wait()

    lane = lax.broadcasted_iota(jnp.int32, (8, LANES), 1)
    pitch = WINDOWS * NY

    def out_copy(c, k, v):
        width = min(LANES, NX - v * LANES)
        slot = lax.rem(c, 2) * DEEP + k
        return pltpu.make_async_copy(
            stage.at[slot, v] if width == LANES else tail.at[slot],
            out_ref.at[c * DEEP + k, :, pl.ds(v * LANES, width)],
            out_sem.at[slot, v],
        )

    def describe(c, item):
        far = sizes[c, 1]
        slot = lax.bitwise_and(item - far, count - 1)
        filled = item < sizes[c, 0] + far
        source = jnp.where(filled, sources[slot] + c * (DEEP * 8 * stride), 0)
        return source, targets[slot] + c * pitch, turns[slot]

    def turned_planes(words):
        source, _, turn = words
        planes = [boxes[pl.ds(source + k * 8 * stride, 8, stride=stride), :] for k in range(DEEP)]
        return [pltpu.roll(plane, turn, 1) for plane in planes]

    def chunk(c, carry):
        total = sizes[c, 0] + sizes[c, 1]
        steps = jnp.maximum((total + UNROLL - 1) // UNROLL, 1)

        def add(words, values):
            base, turn = words
            part = lax.shift_right_logical(lax.bitwise_and(lane - turn, LANES - 1), 5)
            masks = [part == g for g in range(4)]
            for k in range(DEEP):
                for g in range(4):
                    at = pl.ds(base + g, 8, stride=4)
                    accs[k][at, :] = accs[k][at, :] + jnp.where(masks[g], values[k], 0.0)

        def place(step, carry):
            last = step == steps - 1
            after = jnp.where(last, jnp.minimum(c + 1, CHUNKS - 1), c)
            fresh = [describe(c, step * UNROLL + u) for u in range(CARRY, UNROLL)]
            ahead = [describe(after, jnp.where(last, 0, (step + 1) * UNROLL) + u) for u in range(CARRY)]
            turned = [turned_planes(words) for words in fresh + ahead]
            for words, values in zip(carry[0], carry[1]):
                add(words, values)
            for (_, base, turn), values in zip(fresh, turned):
                add((base, turn), values)
            words = [(base, turn) for _, base, turn in ahead]
            return words, turned[UNROLL - CARRY :]

        carry = lax.fori_loop(0, steps, place, carry)

        @pl.when(c >= 2)
        def _():
            for k in range(DEEP):
                for v in range(TILES):
                    out_copy(c - 2, k, v).wait()

        bank = lax.rem(c, 2)
        for k in range(DEEP):
            slot = bank * DEEP + k
            for r in range(4):
                x_of = lax.bitwise_and(lane - 32 * r, LANES - 1)
                for i in range(NY // 32):
                    first = c * pitch + r + 32 * i
                    parts = [accs[k][pl.ds(first + t * NY, 8, stride=4), :] for t in range(WINDOWS)]
                    for v in range(TILES):
                        sum_v = None
                        for t in range(WINDOWS):
                            low = max(STEP * t - LANES * v, 0)
                            high = min(STEP * t + LANES - LANES * v, LANES)
                            if low >= min(high, NX - LANES * v):
                                continue
                            value = parts[t]
                            if low > 0:
                                value = jnp.where(x_of >= low, value, 0.0)
                            elif high < LANES and min(high, NX - LANES * v) == high:
                                value = jnp.where(x_of < high, value, 0.0)
                            sum_v = value if sum_v is None else sum_v + value
                        if r:
                            sum_v = pltpu.roll(sum_v, LANES - 32 * r, 1)
                        at = pl.ds(r + 32 * i, 8, stride=4)
                        if (v + 1) * LANES > NX:
                            tail[slot, at, :] = sum_v[:, :TAIL]
                        else:
                            stage[slot, v, at, :] = sum_v
            for v in range(TILES):
                out_copy(c, k, v).start()
        return carry

    first = [describe(0, u) for u in range(CARRY)]
    turned = [turned_planes(words) for words in first]
    lax.fori_loop(0, CHUNKS, chunk, ([(base, turn) for _, base, turn in first], turned))
    for c in (CHUNKS - 2, CHUNKS - 1):
        for k in range(DEEP):
            for v in range(TILES):
                out_copy(jnp.int32(c), k, v).wait()


def place_boxes(packed, hot, table, counts, shapes, accs, slots):
    stride = 2 * slots + 1
    columns = shapes.shape[1]
    vmem = pl.BlockSpec(memory_space=pltpu.VMEM)
    inputs = (packed, hot, table, counts, shapes, *accs)
    return pl.pallas_call(
        functools.partial(place_kernel, slots, stride),
        out_shape=[
            jax.ShapeDtypeStruct((ZS, NY, NX), jnp.float32),
            *[pltpu.VMEM(acc.shape, acc.dtype) for acc in accs],
        ],
        in_specs=[vmem] * len(inputs),
        out_specs=[pl.BlockSpec(memory_space=pltpu.HBM)] + [vmem] * DEEP,
        input_output_aliases={5 + k: 1 + k for k in range(DEEP)},
        scratch_shapes=[
            pltpu.VMEM(((columns // LANES + 2 * PAD) * stride + 8, LANES), jnp.float32),
            pltpu.VMEM((2 * DEEP, NX // LANES, NY, LANES), jnp.float32),
            pltpu.VMEM((2 * DEEP, NY, max(TAIL, 1)), jnp.float32),
            *[pltpu.SMEM((2 * slots,), jnp.int32)] * 3,
            pltpu.SMEM((CHUNKS, LANES), jnp.int32),
            pltpu.SemaphoreType.DMA((4,)),
            pltpu.SemaphoreType.DMA((2 * DEEP, TILES)),
        ],
        compiler_params=pltpu.CompilerParams(vmem_limit_bytes=30 * 1024 * 1024),
    )(*[pltpu.with_memory_space_constraint(value, pltpu.VMEM) for value in inputs])[0]


def share_kernel(
    bands, slabs, coef_ref, occupation_ref, shapes_ref, corners_ref,
    out_ref, hot_ref, table_ref, counts_ref, shp, *refs,
):
    accs, refs = refs[:DEEP], refs[DEEP:]
    (
    raw, level, plain, heavy, part, parts, mine, rows, load_sem, shape_sem, send_a, recv_a, send_b, recv_b,
    ) = refs
    band = lax.axis_index("band")
    slab = lax.axis_index("grid")
    barrier = pltpu.get_barrier_semaphore()
    mesh_id = pl.DeviceIdType.MESH

    def band_peer(d):
        return (lax.rem(band + d, bands), slab)

    def slab_peer(d):
        return (band, lax.rem(slab + d, slabs))

    peers = [band_peer(d) for d in range(1, bands)] + [slab_peer(d) for d in range(1, slabs)]
    for peer in peers:
        pl.semaphore_signal(barrier, inc=1, device_id=peer, device_id_type=mesh_id)
    loads = [
        pltpu.make_async_copy(occupation_ref, level, load_sem.at[0]),
        pltpu.make_async_copy(coef_ref, raw, load_sem.at[1]),
    ]
    for load in loads:
        load.start()
    shape_load = pltpu.make_async_copy(shapes_ref, shp, shape_sem)
    shape_load.start()
    for load in loads:
        load.wait()
    weight = level[...].astype(jnp.float32) * 0.5

    projectors, atoms, depth = raw.shape
    half = atoms // 2
    for i in range(projectors):
        value = raw[i].astype(jnp.float32)
        plain[i] = value
        heavy[i] = value * weight
    lane = lax.broadcasted_iota(jnp.int32, (1, LANES), 1)
    main = jnp.zeros((atoms, LANES), jnp.float32)
    rest = jnp.zeros((half, LANES), jnp.float32)
    pair = 0
    for i in range(projectors):
        left = plain[i]
        for j in range(i, projectors):
            product = left * heavy[j]
            total = product[:, :LANES]
            for v in range(1, depth // LANES):
                total = total + product[:, v * LANES : (v + 1) * LANES]
            total = jnp.sum(total, axis=1, keepdims=True)
            if i == j:
                total = total * 0.5
            if pair < LANES:
                main = jnp.where(lane == pair, total, main)
            else:
                rest = jnp.where(lane == pair - LANES, total[:half], rest)
                rest = jnp.where(lane == pair - HALF, total[half:], rest)
            pair = pair + 1
    part[:atoms, :] = main
    part[atoms:, :] = rest
    pl.semaphore_wait(barrier, len(peers))

    copies = []
    for d in range(1, bands):
        copy = pltpu.make_async_remote_copy(
            src_ref=part, dst_ref=parts.at[band], send_sem=send_a.at[d - 1],
            recv_sem=recv_a.at[d - 1], device_id=band_peer(d), device_id_type=mesh_id,
        )
        copy.start()
        copies.append(copy)
    parts[band] = part[...]
    zero = jnp.zeros((64, LANES), jnp.float32)

    def clear(i, carry):
        for acc in accs:
            acc[pl.ds(pl.multiple_of(i * 64, 64), 64), :] = zero
        return carry

    lax.fori_loop(0, accs[0].shape[0] // 64, clear, 0)
    for copy in copies:
        copy.wait()
    total = parts[0]
    for b in range(1, bands):
        total = total + parts[b]
    packed = total.astype(jnp.bfloat16)
    mine[...] = packed
    copies = []
    for d in range(1, slabs):
        copy = pltpu.make_async_remote_copy(
            src_ref=mine, dst_ref=rows.at[slab], send_sem=send_b.at[d - 1],
            recv_sem=recv_b.at[d - 1], device_id=slab_peer(d), device_id_type=mesh_id,
        )
        copy.start()
        copies.append(copy)
    rows[slab] = packed
    count = hot_ref.shape[0]
    plan_slots(slab, corners_ref, count, count + 1, hot_ref, table_ref, counts_ref)
    for copy in copies:
        copy.wait()
    out_ref[...] = rows[...]
    shape_load.wait()


def share(coefficients, occupation, shapes, corners, bands, slabs):
    atoms, projectors, depth = coefficients.shape
    lines = atoms + atoms // 2
    slots = 4 * atoms
    f32 = jnp.float32
    vmem = pl.BlockSpec(memory_space=pltpu.VMEM)
    hbm = pl.BlockSpec(memory_space=pltpu.HBM)
    inputs = (jnp.transpose(coefficients, (1, 0, 2)), occupation.reshape(1, depth), shapes)
    return pl.pallas_call(
        functools.partial(share_kernel, bands, slabs),
        out_shape=[
            pltpu.VMEM((slabs, lines, LANES), jnp.bfloat16),
            pltpu.VMEM((slots, corners.shape[1]), jnp.bfloat16),
            pltpu.VMEM((8, slots), jnp.int32),
            pltpu.VMEM((CHUNKS, LANES), jnp.int32),
            pltpu.VMEM(shapes.shape, shapes.dtype),
            *[pltpu.VMEM((CHUNKS * WINDOWS * NY, LANES), f32)] * DEEP,
        ],
        in_specs=[hbm, hbm, hbm, vmem],
        out_specs=[vmem] * (5 + DEEP),
        scratch_shapes=[
            pltpu.VMEM((projectors, atoms, depth), jnp.bfloat16),
            pltpu.VMEM((1, depth), jnp.int32),
            pltpu.VMEM((projectors, atoms, depth), f32),
            pltpu.VMEM((projectors, atoms, depth), f32),
            pltpu.VMEM((lines, LANES), f32),
            pltpu.VMEM((bands, lines, LANES), f32),
            pltpu.VMEM((lines, LANES), jnp.bfloat16),
            pltpu.VMEM((slabs, lines, LANES), jnp.bfloat16),
            pltpu.SemaphoreType.DMA((2,)),
            pltpu.SemaphoreType.DMA,
            pltpu.SemaphoreType.DMA((bands - 1,)),
            pltpu.SemaphoreType.DMA((bands - 1,)),
            pltpu.SemaphoreType.DMA((slabs - 1,)),
            pltpu.SemaphoreType.DMA((slabs - 1,)),
        ],
        compiler_params=pltpu.CompilerParams(
            collective_id=0, has_side_effects=True, vmem_limit_bytes=8 * 1024 * 1024
        ),
    )(*[pltpu.with_memory_space_constraint(value, pltpu.HBM) for value in inputs], corners)


def body(coefficients, occupation, shapes, corners):
    bands, slabs = lax.axis_size("band"), lax.axis_size("grid")
    packed, hot, table, counts, shapes, *accs = share(
        coefficients, occupation, shapes, corners, bands, slabs
    )
    return place_boxes(packed, hot, table, counts, shapes, accs, 2 * coefficients.shape[0])


def solution(mesh):
    placed = (P("grid", None, "band"), P("band"), P(), P())
    return jax.shard_map(
        body, mesh=mesh, in_specs=placed, out_specs=P("grid", None, None), check_vma=False
    )
```

```python
import functools

import jax
import jax.numpy as jnp
from jax import lax
from jax.experimental import pallas as pl
from jax.experimental.pallas import tpu as pltpu
from jax.sharding import PartitionSpec as P

BOX = 32
ZS = 32
NY = 288
NX = 288
LANES = 128
STEP = LANES - BOX
HALF = LANES // 2


WINDOWS = (NX - BOX) // STEP + 1
TILES = -(-NX // LANES)
TAIL = NX % LANES
DEEP = 4
CHUNKS = ZS // DEEP
PAD = 8 * DEEP
UNROLL = 24
CARRY = 4


def plan_slots(slab, corners_ref, count, stride, hot_ref, table_ref, counts_ref):
    atoms = corners_ref.shape[1]

    depth = corners_ref[0:1, :]
    owner = lax.shift_right_logical(depth, ZS.bit_length() - 1)
    local = depth - owner * ZS
    own = owner == slab
    below = jnp.logical_and(owner == slab - 1, local > 0)
    index = lax.broadcasted_iota(jnp.int32, (1, atoms), 1)
    key = jnp.where(own, local, jnp.where(below, ZS + 1 + local, ZS)) * atoms + index
    key = key.astype(jnp.float32)
    slot_rows = []
    for a in range(atoms // LANES):
        mine = key[:, a * LANES : (a + 1) * LANES]
        rank = jnp.zeros((1, LANES), jnp.float32)
        for b in range(atoms // LANES):
            other = jnp.broadcast_to(key[:, b * LANES : (b + 1) * LANES], (LANES, LANES)).T
            rank = rank + jnp.sum((other < mine).astype(jnp.float32), axis=0, keepdims=True)
        slot_rows.append(rank)
    slot_of = jnp.concatenate(slot_rows, axis=1).astype(jnp.int32)
    slot_of = jnp.where(own, slot_of, jnp.where(below, slot_of + (count - atoms), -1))
    hot = lax.broadcasted_iota(jnp.int32, (count, atoms), 0) == slot_of
    hot = hot.astype(jnp.float32).astype(jnp.bfloat16)
    hot_ref[...] = hot
    start = jnp.where(own, -local, ZS - local)
    line = lax.broadcasted_iota(jnp.int32, (8, atoms), 0)
    traits = jnp.where(line == 0, corners_ref[1:2, :], jnp.where(line == 1, corners_ref[2:3, :], start))
    traits = traits.astype(jnp.float32).astype(jnp.bfloat16)
    traits = lax.dot_general(traits, hot, (((1,), (1,)), ((), ())), preferred_element_type=jnp.float32)
    traits = traits.astype(jnp.int32)
    row, column, start = traits[0:1, :], traits[1:2, :], traits[2:3, :]
    window = jnp.zeros_like(column)
    for t in range(1, WINDOWS):
        window = window + (column >= t * STEP).astype(jnp.int32)
    source = (PAD + start * 8) * stride + lax.broadcasted_iota(jnp.int32, (1, count), 1)
    target = window * NY + row
    turn = lax.bitwise_and(column + 32 * row, LANES - 1)
    for at, value in enumerate((source, target, turn)):
        table_ref[at : at + 1, :] = value
    bound = lax.broadcasted_iota(jnp.int32, (CHUNKS, atoms), 0) * DEEP
    near = jnp.sum(jnp.where(jnp.logical_and(own, local < bound + DEEP), 1.0, 0.0), axis=1, keepdims=True)
    far = jnp.sum(jnp.where(jnp.logical_and(below, local > bound), 1.0, 0.0), axis=1, keepdims=True)
    side = lax.broadcasted_iota(jnp.int32, (CHUNKS, LANES), 1)
    counts_ref[...] = jnp.where(side == 0, near, far).astype(jnp.int32)


def place_kernel(
    slots, stride, packed_ref, hot_ref, table_ref, counts_ref, shapes_ref, *refs,
):
    out_ref = refs[DEEP]
    accs = refs[DEEP + 1 : 2 * DEEP + 1]
    boxes, stage, tail, sources, targets, turns, sizes, word_sem, out_sem = refs[2 * DEEP + 1 :]
    columns = shapes_ref.shape[1]
    count = 2 * slots
    atoms = hot_ref.shape[1]
    hot = hot_ref[...]
    word_copies = [
        pltpu.make_async_copy(table_ref.at[0], sources, word_sem.at[0]),
        pltpu.make_async_copy(table_ref.at[1], targets, word_sem.at[1]),
        pltpu.make_async_copy(table_ref.at[2], turns, word_sem.at[2]),
        pltpu.make_async_copy(counts_ref, sizes, word_sem.at[3]),
    ]
    for copy in word_copies:
        copy.start()

    slabs, lines, _ = packed_ref.shape
    share = lines * 2 // 3
    firsts, rests = [], []
    for s in range(slabs):
        firsts.append(packed_ref[s, :share, :])
        rests.extend([packed_ref[s, share:, :]] * 2)
    lane = lax.broadcasted_iota(jnp.int32, (atoms, LANES), 1)
    side = lax.rem(lax.broadcasted_iota(jnp.int32, (atoms, LANES), 0), share) >= share // 2
    rest = jnp.concatenate(rests, axis=0).astype(jnp.float32)
    rest = jnp.where(lane == LANES - 1, side.astype(jnp.float32), rest).astype(jnp.bfloat16)
    first = jnp.dot(hot, jnp.concatenate(firsts, axis=0), preferred_element_type=jnp.float32)
    rest = jnp.dot(hot, rest, preferred_element_type=jnp.float32)
    rest = jnp.where(rest[:, LANES - 1 :] > 0.5, pltpu.roll(rest, HALF, 1), rest)
    pairs = shapes_ref.shape[0]
    rows = jnp.concatenate([first, rest[:, : pairs - LANES]], axis=1).astype(jnp.bfloat16)

    span = 4096
    strip = -(-PAD * stride * span // (8 * columns)) * 8
    zero = jnp.zeros((8, LANES), jnp.float32)

    def multiply(s, carry):
        at = pl.multiple_of(s * span, span)
        product = jnp.dot(rows, shapes_ref[:, pl.ds(at, span)], preferred_element_type=jnp.float32)
        for c in range(span // LANES):
            spot = (PAD + at // LANES + c) * stride
            boxes[pl.ds(spot, count), :] = product[:, c * LANES : (c + 1) * LANES]
        edge = jnp.minimum(s * strip, PAD * stride - strip)
        for u in range(strip // 8):
            boxes[pl.ds(edge + 8 * u, 8), :] = zero
            boxes[pl.ds(edge + (PAD + columns // LANES) * stride + 8 * u, 8), :] = zero
        return carry

    lax.fori_loop(0, columns // span, multiply, 0)
    for copy in word_copies:
        copy.wait()

    lane = lax.broadcasted_iota(jnp.int32, (8, LANES), 1)
    pitch = WINDOWS * NY

    def out_copy(c, k, v):
        width = min(LANES, NX - v * LANES)
        slot = lax.rem(c, 2) * DEEP + k
        return pltpu.make_async_copy(
            stage.at[slot, v] if width == LANES else tail.at[slot],
            out_ref.at[c * DEEP + k, :, pl.ds(v * LANES, width)],
            out_sem.at[slot, v],
        )

    def describe(c, item):
        far = sizes[c, 1]
        slot = lax.bitwise_and(item - far, count - 1)
        filled = item < sizes[c, 0] + far
        source = jnp.where(filled, sources[slot] + c * (DEEP * 8 * stride), 0)
        return source, targets[slot] + c * pitch, turns[slot]

    def turned_planes(words):
        source, _, turn = words
        planes = [boxes[pl.ds(source + k * 8 * stride, 8, stride=stride), :] for k in range(DEEP)]
        return [pltpu.roll(plane, turn, 1) for plane in planes]

    def chunk(c, carry):
        total = sizes[c, 0] + sizes[c, 1]
        steps = jnp.maximum((total + UNROLL - 1) // UNROLL, 1)

        def add(words, values):
            base, turn = words
            part = lax.shift_right_logical(lax.bitwise_and(lane - turn, LANES - 1), 5)
            masks = [jnp.where(part == g, 1.0, 0.0) for g in range(4)]
            for k in range(DEEP):
                for g in range(4):
                    at = pl.ds(base + g, 8, stride=4)
                    accs[k][at, :] = accs[k][at, :] + masks[g] * values[k]

        def place(step, carry):
            last = step == steps - 1
            after = jnp.where(last, jnp.minimum(c + 1, CHUNKS - 1), c)
            fresh = [describe(c, step * UNROLL + u) for u in range(CARRY, UNROLL)]
            ahead = [describe(after, jnp.where(last, 0, (step + 1) * UNROLL) + u) for u in range(CARRY)]
            turned = [turned_planes(words) for words in fresh + ahead]
            for words, values in zip(carry[0], carry[1]):
                add(words, values)
            for (_, base, turn), values in zip(fresh, turned):
                add((base, turn), values)
            words = [(base, turn) for _, base, turn in ahead]
            return words, turned[UNROLL - CARRY :]

        carry = lax.fori_loop(0, steps, place, carry)

        @pl.when(c >= 2)
        def _():
            for k in range(DEEP):
                for v in range(TILES):
                    out_copy(c - 2, k, v).wait()

        bank = lax.rem(c, 2)
        for k in range(DEEP):
            slot = bank * DEEP + k
            for r in range(4):
                x_of = lax.bitwise_and(lane - 32 * r, LANES - 1)
                for i in range(NY // 32):
                    first = c * pitch + r + 32 * i
                    parts = [accs[k][pl.ds(first + t * NY, 8, stride=4), :] for t in range(WINDOWS)]
                    for v in range(TILES):
                        sum_v = None
                        for t in range(WINDOWS):
                            low = max(STEP * t - LANES * v, 0)
                            high = min(STEP * t + LANES - LANES * v, LANES)
                            if low >= min(high, NX - LANES * v):
                                continue
                            value = parts[t]
                            if low > 0:
                                value = jnp.where(x_of >= low, value, 0.0)
                            elif high < LANES and min(high, NX - LANES * v) == high:
                                value = jnp.where(x_of < high, value, 0.0)
                            sum_v = value if sum_v is None else sum_v + value
                        if r:
                            sum_v = pltpu.roll(sum_v, LANES - 32 * r, 1)
                        at = pl.ds(r + 32 * i, 8, stride=4)
                        if (v + 1) * LANES > NX:
                            tail[slot, at, :] = sum_v[:, :TAIL]
                        else:
                            stage[slot, v, at, :] = sum_v
            for v in range(TILES):
                out_copy(c, k, v).start()
        return carry

    first = [describe(0, u) for u in range(CARRY)]
    turned = [turned_planes(words) for words in first]
    lax.fori_loop(0, CHUNKS, chunk, ([(base, turn) for _, base, turn in first], turned))
    for c in (CHUNKS - 2, CHUNKS - 1):
        for k in range(DEEP):
            for v in range(TILES):
                out_copy(jnp.int32(c), k, v).wait()


def place_boxes(packed, hot, table, counts, shapes, accs, slots):
    stride = 2 * slots + 1
    columns = shapes.shape[1]
    vmem = pl.BlockSpec(memory_space=pltpu.VMEM)
    inputs = (packed, hot, table, counts, shapes, *accs)
    return pl.pallas_call(
        functools.partial(place_kernel, slots, stride),
        out_shape=[
            jax.ShapeDtypeStruct((ZS, NY, NX), jnp.float32),
            *[pltpu.VMEM(acc.shape, acc.dtype) for acc in accs],
        ],
        in_specs=[vmem] * len(inputs),
        out_specs=[pl.BlockSpec(memory_space=pltpu.HBM)] + [vmem] * DEEP,
        input_output_aliases={5 + k: 1 + k for k in range(DEEP)},
        scratch_shapes=[
            pltpu.VMEM(((columns // LANES + 2 * PAD) * stride + 8, LANES), jnp.float32),
            pltpu.VMEM((2 * DEEP, NX // LANES, NY, LANES), jnp.float32),
            pltpu.VMEM((2 * DEEP, NY, max(TAIL, 1)), jnp.float32),
            *[pltpu.SMEM((2 * slots,), jnp.int32)] * 3,
            pltpu.SMEM((CHUNKS, LANES), jnp.int32),
            pltpu.SemaphoreType.DMA((4,)),
            pltpu.SemaphoreType.DMA((2 * DEEP, TILES)),
        ],
        compiler_params=pltpu.CompilerParams(vmem_limit_bytes=26 * 1024 * 1024),
    )(*[pltpu.with_memory_space_constraint(value, pltpu.VMEM) for value in inputs])[0]


def share_kernel(
    bands, slabs, coef_ref, occupation_ref, shapes_ref, corners_ref,
    out_ref, hot_ref, table_ref, counts_ref, shp, *refs,
):
    accs, refs = refs[:DEEP], refs[DEEP:]
    (
    raw, level, spots, plain, heavy, part, parts, mine, rows, load_sem, shape_sem, send_a, recv_a, send_b, recv_b,
    ) = refs
    band = lax.axis_index("band")
    slab = lax.axis_index("grid")
    barrier = pltpu.get_barrier_semaphore()
    mesh_id = pl.DeviceIdType.MESH

    def band_peer(d):
        return (lax.rem(band + d, bands), slab)

    def slab_peer(d):
        return (band, lax.rem(slab + d, slabs))

    peers = [band_peer(d) for d in range(1, bands)] + [slab_peer(d) for d in range(1, slabs)]
    for peer in peers:
        pl.semaphore_signal(barrier, inc=1, device_id=peer, device_id_type=mesh_id)
    loads = [
        pltpu.make_async_copy(occupation_ref, level, load_sem.at[0]),
        pltpu.make_async_copy(coef_ref, raw, load_sem.at[1]),
        pltpu.make_async_copy(corners_ref, spots, load_sem.at[2]),
    ]
    for load in loads:
        load.start()
    shape_load = pltpu.make_async_copy(shapes_ref, shp, shape_sem)
    shape_load.start()
    for load in loads:
        load.wait()
    weight = level[...].astype(jnp.float32) * 0.5

    projectors, atoms, depth = raw.shape
    half = atoms // 2
    for i in range(projectors):
        value = raw[i].astype(jnp.float32)
        plain[i] = value
        heavy[i] = value * weight
    lane = lax.broadcasted_iota(jnp.int32, (1, LANES), 1)
    main = jnp.zeros((atoms, LANES), jnp.float32)
    rest = jnp.zeros((half, LANES), jnp.float32)
    pair = 0
    for i in range(projectors):
        left = plain[i]
        for j in range(i, projectors):
            product = left * heavy[j]
            total = product[:, :LANES]
            for v in range(1, depth // LANES):
                total = total + product[:, v * LANES : (v + 1) * LANES]
            total = jnp.sum(total, axis=1, keepdims=True)
            if i == j:
                total = total * 0.5
            if pair < LANES:
                main = jnp.where(lane == pair, total, main)
            else:
                rest = jnp.where(lane == pair - LANES, total[:half], rest)
                rest = jnp.where(lane == pair - HALF, total[half:], rest)
            pair = pair + 1
    part[:atoms, :] = main
    part[atoms:, :] = rest
    pl.semaphore_wait(barrier, len(peers))

    copies = []
    for d in range(1, bands):
        copy = pltpu.make_async_remote_copy(
            src_ref=part, dst_ref=parts.at[band], send_sem=send_a.at[d - 1],
            recv_sem=recv_a.at[d - 1], device_id=band_peer(d), device_id_type=mesh_id,
        )
        copy.start()
        copies.append(copy)
    parts[band] = part[...]
    zero = jnp.zeros((64, LANES), jnp.float32)

    def clear(i, carry):
        for acc in accs:
            acc[pl.ds(pl.multiple_of(i * 64, 64), 64), :] = zero
        return carry

    lax.fori_loop(0, accs[0].shape[0] // 64, clear, 0)
    for copy in copies:
        copy.wait()
    total = parts[0]
    for b in range(1, bands):
        total = total + parts[b]
    packed = total.astype(jnp.bfloat16)
    mine[...] = packed
    copies = []
    for d in range(1, slabs):
        copy = pltpu.make_async_remote_copy(
            src_ref=mine, dst_ref=rows.at[slab], send_sem=send_b.at[d - 1],
            recv_sem=recv_b.at[d - 1], device_id=slab_peer(d), device_id_type=mesh_id,
        )
        copy.start()
        copies.append(copy)
    rows[slab] = packed
    count = hot_ref.shape[0]
    plan_slots(slab, spots, count, count + 1, hot_ref, table_ref, counts_ref)
    for copy in copies:
        copy.wait()
    out_ref[...] = rows[...]
    shape_load.wait()


def share(coefficients, occupation, shapes, corners, bands, slabs):
    atoms, projectors, depth = coefficients.shape
    lines = atoms + atoms // 2
    slots = 4 * atoms
    f32 = jnp.float32
    vmem = pl.BlockSpec(memory_space=pltpu.VMEM)
    hbm = pl.BlockSpec(memory_space=pltpu.HBM)
    inputs = (jnp.transpose(coefficients, (1, 0, 2)), occupation.reshape(1, depth), shapes, corners)
    return pl.pallas_call(
        functools.partial(share_kernel, bands, slabs),
        out_shape=[
            pltpu.VMEM((slabs, lines, LANES), jnp.bfloat16),
            pltpu.VMEM((slots, corners.shape[1]), jnp.bfloat16),
            pltpu.VMEM((8, slots), jnp.int32),
            pltpu.VMEM((CHUNKS, LANES), jnp.int32),
            pltpu.VMEM(shapes.shape, shapes.dtype),
            *[pltpu.VMEM((CHUNKS * WINDOWS * NY, LANES), f32)] * DEEP,
        ],
        in_specs=[hbm] * 4,
        out_specs=[vmem] * (5 + DEEP),
        scratch_shapes=[
            pltpu.VMEM((projectors, atoms, depth), jnp.bfloat16),
            pltpu.VMEM((1, depth), jnp.int32),
            pltpu.VMEM(corners.shape, jnp.int32),
            pltpu.VMEM((projectors, atoms, depth), f32),
            pltpu.VMEM((projectors, atoms, depth), f32),
            pltpu.VMEM((lines, LANES), f32),
            pltpu.VMEM((bands, lines, LANES), f32),
            pltpu.VMEM((lines, LANES), jnp.bfloat16),
            pltpu.VMEM((slabs, lines, LANES), jnp.bfloat16),
            pltpu.SemaphoreType.DMA((3,)),
            pltpu.SemaphoreType.DMA,
            pltpu.SemaphoreType.DMA((bands - 1,)),
            pltpu.SemaphoreType.DMA((bands - 1,)),
            pltpu.SemaphoreType.DMA((slabs - 1,)),
            pltpu.SemaphoreType.DMA((slabs - 1,)),
        ],
        compiler_params=pltpu.CompilerParams(
            collective_id=0, has_side_effects=True, vmem_limit_bytes=8 * 1024 * 1024
        ),
    )(*[pltpu.with_memory_space_constraint(value, pltpu.HBM) for value in inputs])


def body(coefficients, occupation, shapes, corners):
    bands, slabs = lax.axis_size("band"), lax.axis_size("grid")
    packed, hot, table, counts, shapes, *accs = share(
        coefficients, occupation, shapes, corners, bands, slabs
    )
    return place_boxes(packed, hot, table, counts, shapes, accs, 2 * coefficients.shape[0])


def solution(mesh):
    placed = (P("grid", None, "band"), P("band"), P(), P())
    return jax.shard_map(
        body, mesh=mesh, in_specs=placed, out_specs=P("grid", None, None), check_vma=False
    )
```

```python
import functools

import jax
import jax.numpy as jnp
from jax import lax
from jax.experimental import pallas as pl
from jax.experimental.pallas import tpu as pltpu
from jax.sharding import PartitionSpec as P

BOX = 32
ZS = 32
NY = 288
NX = 288
LANES = 128
STEP = LANES - BOX
HALF = LANES // 2


WINDOWS = (NX - BOX) // STEP + 1
TILES = -(-NX // LANES)
TAIL = NX % LANES
DEEP = 4
CHUNKS = ZS // DEEP
PAD = 8 * DEEP
UNROLL = 24
CARRY = 4


def plan_slots(slab, corners_ref, count, stride, hot_ref, table_ref, counts_ref):
    atoms = corners_ref.shape[1]

    depth = corners_ref[0:1, :]
    owner = lax.shift_right_logical(depth, ZS.bit_length() - 1)
    local = depth - owner * ZS
    own = owner == slab
    below = jnp.logical_and(owner == slab - 1, local > 0)
    index = lax.broadcasted_iota(jnp.int32, (1, atoms), 1)
    key = jnp.where(own, local, jnp.where(below, ZS + 1 + local, ZS)) * atoms + index
    key = key.astype(jnp.float32)
    slot_rows = []
    for a in range(atoms // LANES):
        mine = key[:, a * LANES : (a + 1) * LANES]
        rank = jnp.zeros((1, LANES), jnp.float32)
        for b in range(atoms // LANES):
            other = jnp.broadcast_to(key[:, b * LANES : (b + 1) * LANES], (LANES, LANES)).T
            rank = rank + jnp.sum((other < mine).astype(jnp.float32), axis=0, keepdims=True)
        slot_rows.append(rank)
    slot_of = jnp.concatenate(slot_rows, axis=1).astype(jnp.int32)
    slot_of = jnp.where(own, slot_of, jnp.where(below, slot_of + (count - atoms), -1))
    hot = lax.broadcasted_iota(jnp.int32, (count, atoms), 0) == slot_of
    hot = hot.astype(jnp.float32).astype(jnp.bfloat16)
    hot_ref[...] = hot
    start = jnp.where(own, -local, ZS - local)
    line = lax.broadcasted_iota(jnp.int32, (8, atoms), 0)
    traits = jnp.where(line == 0, corners_ref[1:2, :], jnp.where(line == 1, corners_ref[2:3, :], start))
    traits = traits.astype(jnp.float32).astype(jnp.bfloat16)
    traits = lax.dot_general(traits, hot, (((1,), (1,)), ((), ())), preferred_element_type=jnp.float32)
    traits = traits.astype(jnp.int32)
    row, column, start = traits[0:1, :], traits[1:2, :], traits[2:3, :]
    window = jnp.zeros_like(column)
    for t in range(1, WINDOWS):
        window = window + (column >= t * STEP).astype(jnp.int32)
    source = (PAD + start * 8) * stride + lax.broadcasted_iota(jnp.int32, (1, count), 1)
    target = window * NY + row
    turn = lax.bitwise_and(column + 32 * row, LANES - 1)
    for at, value in enumerate((source, target, turn)):
        table_ref[at : at + 1, :] = value
    bound = lax.broadcasted_iota(jnp.int32, (CHUNKS, atoms), 0) * DEEP
    near = jnp.sum(jnp.where(jnp.logical_and(own, local < bound + DEEP), 1.0, 0.0), axis=1, keepdims=True)
    far = jnp.sum(jnp.where(jnp.logical_and(below, local > bound), 1.0, 0.0), axis=1, keepdims=True)
    side = lax.broadcasted_iota(jnp.int32, (CHUNKS, LANES), 1)
    counts_ref[...] = jnp.where(side == 0, near, far).astype(jnp.int32)


def place_kernel(
    slots, stride, packed_ref, hot_ref, table_ref, counts_ref, shapes_ref, *refs,
):
    out_ref = refs[DEEP + 1]
    boxes, *accs = refs[DEEP + 2 : 2 * DEEP + 3]
    stage, tail, sources, targets, turns, sizes, word_sem, out_sem = refs[2 * DEEP + 3 :]
    columns = shapes_ref.shape[1]
    count = 2 * slots
    atoms = hot_ref.shape[1]
    hot = hot_ref[...]
    word_copies = [
        pltpu.make_async_copy(table_ref.at[0], sources, word_sem.at[0]),
        pltpu.make_async_copy(table_ref.at[1], targets, word_sem.at[1]),
        pltpu.make_async_copy(table_ref.at[2], turns, word_sem.at[2]),
        pltpu.make_async_copy(counts_ref, sizes, word_sem.at[3]),
    ]
    for copy in word_copies:
        copy.start()

    slabs, lines, _ = packed_ref.shape
    share = lines * 2 // 3
    firsts, rests = [], []
    for s in range(slabs):
        firsts.append(packed_ref[s, :share, :])
        rests.extend([packed_ref[s, share:, :]] * 2)
    lane = lax.broadcasted_iota(jnp.int32, (atoms, LANES), 1)
    side = lax.rem(lax.broadcasted_iota(jnp.int32, (atoms, LANES), 0), share) >= share // 2
    rest = jnp.concatenate(rests, axis=0).astype(jnp.float32)
    rest = jnp.where(lane == LANES - 1, side.astype(jnp.float32), rest).astype(jnp.bfloat16)
    first = jnp.dot(hot, jnp.concatenate(firsts, axis=0), preferred_element_type=jnp.float32)
    rest = jnp.dot(hot, rest, preferred_element_type=jnp.float32)
    rest = jnp.where(rest[:, LANES - 1 :] > 0.5, pltpu.roll(rest, HALF, 1), rest)
    pairs = shapes_ref.shape[0]
    rows = jnp.concatenate([first, rest[:, : pairs - LANES]], axis=1).astype(jnp.bfloat16)

    span = 4096

    def multiply(s, carry):
        at = pl.multiple_of(s * span, span)
        product = jnp.dot(rows, shapes_ref[:, pl.ds(at, span)], preferred_element_type=jnp.float32)
        for c in range(span // LANES):
            spot = (PAD + at // LANES + c) * stride
            boxes[pl.ds(spot, count), :] = product[:, c * LANES : (c + 1) * LANES]
        return carry

    lax.fori_loop(0, columns // span, multiply, 0)
    for copy in word_copies:
        copy.wait()

    lane = lax.broadcasted_iota(jnp.int32, (8, LANES), 1)
    pitch = WINDOWS * NY
    come = lax.bitwise_and(lax.broadcasted_iota(jnp.int32, (2 * LANES, 3 * LANES), 0), LANES - 1)
    goes = lax.broadcasted_iota(jnp.int32, (2 * LANES, 3 * LANES), 1)
    goes = lax.bitwise_and(goes, LANES - 1) + 32 * (lax.shift_right_logical(goes, 7) + 1)
    move = jnp.where(come == goes, 1.0, 0.0).astype(jnp.bfloat16)

    def out_copy(c, k, v):
        width = min(LANES, NX - v * LANES)
        slot = lax.rem(c, 2) * DEEP + k
        return pltpu.make_async_copy(
            stage.at[slot, v] if width == LANES else tail.at[slot],
            out_ref.at[c * DEEP + k, :, pl.ds(v * LANES, width)],
            out_sem.at[slot, v],
        )

    def describe(c, item):
        far = sizes[c, 1]
        slot = lax.bitwise_and(item - far, count - 1)
        filled = item < sizes[c, 0] + far
        source = jnp.where(filled, sources[slot] + c * (DEEP * 8 * stride), 0)
        return source, targets[slot] + c * pitch, turns[slot]

    def turned_planes(words):
        source, _, turn = words
        planes = [boxes[pl.ds(source + k * 8 * stride, 8, stride=stride), :] for k in range(DEEP)]
        return [pltpu.roll(plane, turn, 1) for plane in planes]

    def chunk(c, carry):
        total = sizes[c, 0] + sizes[c, 1]
        steps = jnp.maximum((total + UNROLL - 1) // UNROLL, 1)

        def add(words, values):
            base, turn = words
            part = lax.shift_right_logical(lax.bitwise_and(lane - turn, LANES - 1), 5)
            masks = [jnp.where(part == g, 1.0, 0.0) for g in range(4)]
            for k in range(DEEP):
                for g in range(4):
                    at = pl.ds(base + g, 8, stride=4)
                    accs[k][at, :] = accs[k][at, :] + masks[g] * values[k]

        def place(step, carry):
            last = step == steps - 1
            after = jnp.where(last, jnp.minimum(c + 1, CHUNKS - 1), c)
            fresh = [describe(c, step * UNROLL + u) for u in range(CARRY, UNROLL)]
            ahead = [describe(after, jnp.where(last, 0, (step + 1) * UNROLL) + u) for u in range(CARRY)]
            turned = [turned_planes(words) for words in fresh + ahead]
            for words, values in zip(carry[0], carry[1]):
                add(words, values)
            for (_, base, turn), values in zip(fresh, turned):
                add((base, turn), values)
            words = [(base, turn) for _, base, turn in ahead]
            return words, turned[UNROLL - CARRY :]

        carry = lax.fori_loop(0, steps, place, carry)

        @pl.when(c >= 2)
        def _():
            for k in range(DEEP):
                for v in range(TILES):
                    out_copy(c - 2, k, v).wait()

        bank = lax.rem(c, 2)
        ends = []
        for k in range(DEEP):
            for i in range(NY // 32):
                first = c * pitch + (WINDOWS - 1) * NY + 32 * i
                end = accs[k][pl.ds(first, 8, stride=4), :]
                for r in range(1, 4):
                    end = jnp.where(lane >= 32 * r, accs[k][pl.ds(first + r, 8, stride=4), :], end)
                tail[bank * DEEP + k, pl.ds(32 * i, 8, stride=4), :] = end[:, :TAIL]
                ends.append(end)
        end = jnp.concatenate(ends, axis=0)
        high = end.astype(jnp.bfloat16)
        low = (end - high.astype(jnp.float32)).astype(jnp.bfloat16)
        moved = jnp.dot(jnp.concatenate([high, low], axis=1), move, preferred_element_type=jnp.float32)
        for k in range(DEEP):
            for i in range(NY // 32):
                for r in range(1, 4):
                    first = k * (NY // 4) + 8 * i
                    value = moved[first : first + 8, (r - 1) * LANES : (r - 1) * LANES + TAIL]
                    tail[bank * DEEP + k, pl.ds(r + 32 * i, 8, stride=4), :] = value
        for k in range(DEEP):
            for i in range(NY // 32):
                for r in range(4):
                    x_of = lax.bitwise_and(lane - 32 * r, LANES - 1)
                    first = c * pitch + r + 32 * i
                    parts = [accs[k][pl.ds(first + t * NY, 8, stride=4), :] for t in range(WINDOWS)]
                    for v in range(NX // LANES):
                        sum_v = None
                        for t in range(WINDOWS):
                            low = max(STEP * t - LANES * v, 0)
                            high = min(STEP * t + LANES - LANES * v, LANES)
                            if low >= high:
                                continue
                            value = parts[t]
                            if low > 0:
                                value = jnp.where(x_of >= low, value, 0.0)
                            elif high < LANES:
                                value = jnp.where(x_of < high, value, 0.0)
                            sum_v = value if sum_v is None else sum_v + value
                        if r:
                            sum_v = pltpu.roll(sum_v, LANES - 32 * r, 1)
                        stage[bank * DEEP + k, v, pl.ds(r + 32 * i, 8, stride=4), :] = sum_v
            for v in range(TILES):
                out_copy(c, k, v).start()
        return carry

    first = [describe(0, u) for u in range(CARRY)]
    turned = [turned_planes(words) for words in first]
    lax.fori_loop(0, CHUNKS, chunk, ([(base, turn) for _, base, turn in first], turned))
    for c in (CHUNKS - 2, CHUNKS - 1):
        for k in range(DEEP):
            for v in range(TILES):
                out_copy(jnp.int32(c), k, v).wait()


def place_boxes(packed, hot, table, counts, shapes, sums, slots):
    stride = 2 * slots + 1
    vmem = pl.BlockSpec(memory_space=pltpu.VMEM)
    inputs = (packed, hot, table, counts, shapes, *sums)
    return pl.pallas_call(
        functools.partial(place_kernel, slots, stride),
        out_shape=[
            jax.ShapeDtypeStruct((ZS, NY, NX), jnp.float32),
            *[pltpu.VMEM(value.shape, value.dtype) for value in sums],
        ],
        in_specs=[vmem] * len(inputs),
        out_specs=[pl.BlockSpec(memory_space=pltpu.HBM)] + [vmem] * (1 + DEEP),
        input_output_aliases={5 + k: 1 + k for k in range(1 + DEEP)},
        scratch_shapes=[
            pltpu.VMEM((2 * DEEP, NX // LANES, NY, LANES), jnp.float32),
            pltpu.VMEM((2 * DEEP, NY, max(TAIL, 1)), jnp.float32),
            *[pltpu.SMEM((2 * slots,), jnp.int32)] * 3,
            pltpu.SMEM((CHUNKS, LANES), jnp.int32),
            pltpu.SemaphoreType.DMA((4,)),
            pltpu.SemaphoreType.DMA((2 * DEEP, TILES)),
        ],
        compiler_params=pltpu.CompilerParams(vmem_limit_bytes=6 * 1024 * 1024),
    )(*[pltpu.with_memory_space_constraint(value, pltpu.VMEM) for value in inputs])[0]


def share_kernel(
    bands, slabs, coef_ref, occupation_ref, shapes_ref, corners_ref,
    out_ref, hot_ref, table_ref, counts_ref, shp, boxes, *refs,
):
    accs, refs = refs[:DEEP], refs[DEEP:]
    (
    raw, level, spots, plain, heavy, part, parts, mine, rows, load_sem, shape_sem, send_a, recv_a, send_b, recv_b,
    ) = refs
    band = lax.axis_index("band")
    slab = lax.axis_index("grid")
    barrier = pltpu.get_barrier_semaphore()
    mesh_id = pl.DeviceIdType.MESH

    def band_peer(d):
        return (lax.rem(band + d, bands), slab)

    def slab_peer(d):
        return (band, lax.rem(slab + d, slabs))

    peers = [band_peer(d) for d in range(1, bands)] + [slab_peer(d) for d in range(1, slabs)]
    for peer in peers:
        pl.semaphore_signal(barrier, inc=1, device_id=peer, device_id_type=mesh_id)
    loads = [
        pltpu.make_async_copy(occupation_ref, level, load_sem.at[0]),
        pltpu.make_async_copy(coef_ref, raw, load_sem.at[1]),
        pltpu.make_async_copy(corners_ref, spots, load_sem.at[2]),
    ]
    for load in loads:
        load.start()
    shape_load = pltpu.make_async_copy(shapes_ref, shp, shape_sem)
    shape_load.start()
    for load in loads:
        load.wait()
    weight = level[...].astype(jnp.float32) * 0.5

    projectors, atoms, depth = raw.shape
    half = atoms // 2
    for i in range(projectors):
        value = raw[i].astype(jnp.float32)
        plain[i] = value
        heavy[i] = value * weight
    lane = lax.broadcasted_iota(jnp.int32, (1, LANES), 1)
    main = jnp.zeros((atoms, LANES), jnp.float32)
    rest = jnp.zeros((half, LANES), jnp.float32)
    pair = 0
    for i in range(projectors):
        left = plain[i]
        for j in range(i, projectors):
            product = left * heavy[j]
            total = product[:, :LANES]
            for v in range(1, depth // LANES):
                total = total + product[:, v * LANES : (v + 1) * LANES]
            total = jnp.sum(total, axis=1, keepdims=True)
            if i == j:
                total = total * 0.5
            if pair < LANES:
                main = jnp.where(lane == pair, total, main)
            else:
                rest = jnp.where(lane == pair - LANES, total[:half], rest)
                rest = jnp.where(lane == pair - HALF, total[half:], rest)
            pair = pair + 1
    part[:atoms, :] = main
    part[atoms:, :] = rest
    pl.semaphore_wait(barrier, len(peers))

    copies = []
    for d in range(1, bands):
        copy = pltpu.make_async_remote_copy(
            src_ref=part, dst_ref=parts.at[band], send_sem=send_a.at[d - 1],
            recv_sem=recv_a.at[d - 1], device_id=band_peer(d), device_id_type=mesh_id,
        )
        copy.start()
        copies.append(copy)
    parts[band] = part[...]
    zero = jnp.zeros((64, LANES), jnp.float32)

    def clear(i, carry):
        for acc in accs:
            acc[pl.ds(pl.multiple_of(i * 64, 64), 64), :] = zero
        return carry

    lax.fori_loop(0, accs[0].shape[0] // 64, clear, 0)
    border = PAD * (hot_ref.shape[0] + 1)

    def clear_border(i, carry):
        for edge in (0, boxes.shape[0] - border):
            boxes[pl.ds(pl.multiple_of(edge + i * 32, 8), 32), :] = zero[:32]
        return carry

    lax.fori_loop(0, border // 32, clear_border, 0)
    for copy in copies:
        copy.wait()
    total = parts[0]
    for b in range(1, bands):
        total = total + parts[b]
    packed = total.astype(jnp.bfloat16)
    mine[...] = packed
    copies = []
    for d in range(1, slabs):
        copy = pltpu.make_async_remote_copy(
            src_ref=mine, dst_ref=rows.at[slab], send_sem=send_b.at[d - 1],
            recv_sem=recv_b.at[d - 1], device_id=slab_peer(d), device_id_type=mesh_id,
        )
        copy.start()
        copies.append(copy)
    rows[slab] = packed
    count = hot_ref.shape[0]
    plan_slots(slab, spots, count, count + 1, hot_ref, table_ref, counts_ref)
    for copy in copies:
        copy.wait()
    out_ref[...] = rows[...]
    shape_load.wait()


def share(coefficients, occupation, shapes, corners, bands, slabs):
    atoms, projectors, depth = coefficients.shape
    lines = atoms + atoms // 2
    slots = 4 * atoms
    f32 = jnp.float32
    vmem = pl.BlockSpec(memory_space=pltpu.VMEM)
    hbm = pl.BlockSpec(memory_space=pltpu.HBM)
    inputs = (jnp.transpose(coefficients, (1, 0, 2)), occupation.reshape(1, depth), shapes, corners)
    return pl.pallas_call(
        functools.partial(share_kernel, bands, slabs),
        out_shape=[
            pltpu.VMEM((slabs, lines, LANES), jnp.bfloat16),
            pltpu.VMEM((slots, corners.shape[1]), jnp.bfloat16),
            pltpu.VMEM((8, slots), jnp.int32),
            pltpu.VMEM((CHUNKS, LANES), jnp.int32),
            pltpu.VMEM(shapes.shape, shapes.dtype),
            pltpu.VMEM(((shapes.shape[1] // LANES + 2 * PAD) * (slots + 1), LANES), f32),
            *[pltpu.VMEM((CHUNKS * WINDOWS * NY, LANES), f32)] * DEEP,
        ],
        in_specs=[hbm] * 4,
        out_specs=[vmem] * (6 + DEEP),
        scratch_shapes=[
            pltpu.VMEM((projectors, atoms, depth), jnp.bfloat16),
            pltpu.VMEM((1, depth), jnp.int32),
            pltpu.VMEM(corners.shape, jnp.int32),
            pltpu.VMEM((projectors, atoms, depth), f32),
            pltpu.VMEM((projectors, atoms, depth), f32),
            pltpu.VMEM((lines, LANES), f32),
            pltpu.VMEM((bands, lines, LANES), f32),
            pltpu.VMEM((lines, LANES), jnp.bfloat16),
            pltpu.VMEM((slabs, lines, LANES), jnp.bfloat16),
            pltpu.SemaphoreType.DMA((3,)),
            pltpu.SemaphoreType.DMA,
            pltpu.SemaphoreType.DMA((bands - 1,)),
            pltpu.SemaphoreType.DMA((bands - 1,)),
            pltpu.SemaphoreType.DMA((slabs - 1,)),
            pltpu.SemaphoreType.DMA((slabs - 1,)),
        ],
        compiler_params=pltpu.CompilerParams(
            collective_id=0, has_side_effects=True, vmem_limit_bytes=6 * 1024 * 1024
        ),
    )(*[pltpu.with_memory_space_constraint(value, pltpu.HBM) for value in inputs])


def body(coefficients, occupation, shapes, corners):
    bands, slabs = lax.axis_size("band"), lax.axis_size("grid")
    packed, hot, table, counts, shapes, *sums = share(
        coefficients, occupation, shapes, corners, bands, slabs
    )
    return place_boxes(packed, hot, table, counts, shapes, sums, 2 * coefficients.shape[0])


def solution(mesh):
    placed = (P("grid", None, "band"), P("band"), P(), P())
    return jax.shard_map(
        body, mesh=mesh, in_specs=placed, out_specs=P("grid", None, None), check_vma=False
    )
```

```python
import functools

import jax
import jax.numpy as jnp
from jax import lax
from jax.experimental import pallas as pl
from jax.experimental.pallas import tpu as pltpu
from jax.sharding import PartitionSpec as P

BOX = 32
ZS = 32
NY = 288
NX = 288
LANES = 128
STEP = LANES - BOX
HALF = LANES // 2


WINDOWS = (NX - BOX) // STEP + 1
TILES = -(-NX // LANES)
TAIL = NX % LANES
DEEP = 4
CHUNKS = ZS // DEEP
PAD = 8 * DEEP
UNROLL = 24
CARRY = 4


def plan_slots(slab, corners_ref, count, stride, hot_ref, table_ref, counts_ref):
    atoms = corners_ref.shape[1]

    depth = corners_ref[0:1, :]
    owner = lax.shift_right_logical(depth, ZS.bit_length() - 1)
    local = depth - owner * ZS
    own = owner == slab
    below = jnp.logical_and(owner == slab - 1, local > 0)
    index = lax.broadcasted_iota(jnp.int32, (1, atoms), 1)
    key = jnp.where(own, local, jnp.where(below, ZS + 1 + local, ZS)) * atoms + index
    key = key.astype(jnp.float32)
    slot_rows = []
    for a in range(atoms // LANES):
        mine = key[:, a * LANES : (a + 1) * LANES]
        rank = jnp.zeros((1, LANES), jnp.float32)
        for b in range(atoms // LANES):
            other = jnp.broadcast_to(key[:, b * LANES : (b + 1) * LANES], (LANES, LANES)).T
            rank = rank + jnp.sum((other < mine).astype(jnp.float32), axis=0, keepdims=True)
        slot_rows.append(rank)
    slot_of = jnp.concatenate(slot_rows, axis=1).astype(jnp.int32)
    slot_of = jnp.where(own, slot_of, jnp.where(below, slot_of + (count - atoms), -1))
    hot = lax.broadcasted_iota(jnp.int32, (count, atoms), 0) == slot_of
    hot = hot.astype(jnp.float32).astype(jnp.bfloat16)
    hot_ref[...] = hot
    start = jnp.where(own, -local, ZS - local)
    line = lax.broadcasted_iota(jnp.int32, (8, atoms), 0)
    traits = jnp.where(line == 0, corners_ref[1:2, :], jnp.where(line == 1, corners_ref[2:3, :], start))
    traits = traits.astype(jnp.float32).astype(jnp.bfloat16)
    traits = lax.dot_general(traits, hot, (((1,), (1,)), ((), ())), preferred_element_type=jnp.float32)
    traits = traits.astype(jnp.int32)
    row, column, start = traits[0:1, :], traits[1:2, :], traits[2:3, :]
    window = jnp.zeros_like(column)
    for t in range(1, WINDOWS):
        window = window + (column >= t * STEP).astype(jnp.int32)
    source = (PAD + start * 8) * stride + lax.broadcasted_iota(jnp.int32, (1, count), 1)
    target = window * NY + row
    turn = lax.bitwise_and(column + 32 * row, LANES - 1)
    for at, value in enumerate((source, target, turn)):
        table_ref[at : at + 1, :] = value
    bound = lax.broadcasted_iota(jnp.int32, (CHUNKS, atoms), 0) * DEEP
    near = jnp.sum(jnp.where(jnp.logical_and(own, local < bound + DEEP), 1.0, 0.0), axis=1, keepdims=True)
    far = jnp.sum(jnp.where(jnp.logical_and(below, local > bound), 1.0, 0.0), axis=1, keepdims=True)
    side = lax.broadcasted_iota(jnp.int32, (CHUNKS, LANES), 1)
    counts_ref[...] = jnp.where(side == 0, near, far).astype(jnp.int32)


def place_kernel(
    slots, stride, packed_ref, hot_ref, table_ref, counts_ref, shapes_ref, *refs,
):
    out_ref = refs[DEEP + 1]
    boxes, *accs = refs[DEEP + 2 : 2 * DEEP + 3]
    stage, tail, sources, targets, turns, sizes, word_sem, out_sem = refs[2 * DEEP + 3 :]
    columns = shapes_ref.shape[1]
    count = 2 * slots
    atoms = hot_ref.shape[1]
    hot = hot_ref[...]
    word_copies = [
        pltpu.make_async_copy(table_ref.at[0], sources, word_sem.at[0]),
        pltpu.make_async_copy(table_ref.at[1], targets, word_sem.at[1]),
        pltpu.make_async_copy(table_ref.at[2], turns, word_sem.at[2]),
        pltpu.make_async_copy(counts_ref, sizes, word_sem.at[3]),
    ]
    for copy in word_copies:
        copy.start()

    slabs, lines, _ = packed_ref.shape
    share = lines * 2 // 3
    firsts, rests = [], []
    for s in range(slabs):
        firsts.append(packed_ref[s, :share, :])
        rests.extend([packed_ref[s, share:, :]] * 2)
    lane = lax.broadcasted_iota(jnp.int32, (atoms, LANES), 1)
    side = lax.rem(lax.broadcasted_iota(jnp.int32, (atoms, LANES), 0), share) >= share // 2
    rest = jnp.concatenate(rests, axis=0).astype(jnp.float32)
    rest = jnp.where(lane == LANES - 1, side.astype(jnp.float32), rest).astype(jnp.bfloat16)
    first = jnp.dot(hot, jnp.concatenate(firsts, axis=0), preferred_element_type=jnp.float32)
    rest = jnp.dot(hot, rest, preferred_element_type=jnp.float32)
    rest = jnp.where(rest[:, LANES - 1 :] > 0.5, pltpu.roll(rest, HALF, 1), rest)
    pairs = shapes_ref.shape[0]
    rows = jnp.concatenate([first, rest[:, : pairs - LANES]], axis=1).astype(jnp.bfloat16)

    span = 16384

    def multiply(s, carry):
        at = pl.multiple_of(s * span, span)
        for part in range(span // 1024):
            product = jnp.dot(
                rows, shapes_ref[:, pl.ds(at + part * 1024, 1024)], preferred_element_type=jnp.float32
            )
            for c in range(1024 // LANES):
                spot = (PAD + at // LANES + part * 1024 // LANES + c) * stride
                boxes[pl.ds(spot, count), :] = product[:, c * LANES : (c + 1) * LANES]
        return carry

    lax.fori_loop(0, columns // span, multiply, 0)
    for copy in word_copies:
        copy.wait()

    lane = lax.broadcasted_iota(jnp.int32, (8, LANES), 1)
    pitch = WINDOWS * NY
    come = lax.bitwise_and(lax.broadcasted_iota(jnp.int32, (2 * LANES, 3 * LANES), 0), LANES - 1)
    goes = lax.broadcasted_iota(jnp.int32, (2 * LANES, 3 * LANES), 1)
    goes = lax.bitwise_and(goes, LANES - 1) + 32 * (lax.shift_right_logical(goes, 7) + 1)
    move = jnp.where(come == goes, 1.0, 0.0).astype(jnp.bfloat16)

    def out_copy(c, k, v):
        width = min(LANES, NX - v * LANES)
        slot = lax.rem(c, 2) * DEEP + k
        return pltpu.make_async_copy(
            stage.at[slot, v] if width == LANES else tail.at[slot],
            out_ref.at[c * DEEP + k, :, pl.ds(v * LANES, width)],
            out_sem.at[slot, v],
        )

    def describe(c, item):
        far = sizes[c, 1]
        slot = lax.bitwise_and(item - far, count - 1)
        filled = item < sizes[c, 0] + far
        source = jnp.where(filled, sources[slot] + c * (DEEP * 8 * stride), 0)
        return source, targets[slot] + c * pitch, turns[slot]

    def turned_planes(words):
        source, _, turn = words
        planes = [boxes[pl.ds(source + k * 8 * stride, 8, stride=stride), :] for k in range(DEEP)]
        return [pltpu.roll(plane, turn, 1) for plane in planes]

    def chunk(c, carry):
        total = sizes[c, 0] + sizes[c, 1]
        halves = jnp.maximum((total + UNROLL // 2 - 1) // (UNROLL // 2), 1)
        many = lax.shift_right_logical(halves, 1)
        few = lax.bitwise_and(halves, 1)

        def add(words, values):
            base, turn = words
            part = lax.shift_right_logical(lax.bitwise_and(lane - turn, LANES - 1), 5)
            masks = [jnp.where(part == g, 1.0, 0.0) for g in range(4)]
            for k in range(DEEP):
                for g in range(4):
                    at = pl.ds(base + g, 8, stride=4)
                    accs[k][at, :] = accs[k][at, :] + masks[g] * values[k]

        def place(begin, size, last, carry):
            after = jnp.where(last, jnp.minimum(c + 1, CHUNKS - 1), c)
            fresh = [describe(c, begin + u) for u in range(CARRY, size)]
            ahead = [describe(after, jnp.where(last, 0, begin + size) + u) for u in range(CARRY)]
            turned = [turned_planes(words) for words in fresh + ahead]
            for words, values in zip(carry[0], carry[1]):
                add(words, values)
            for (_, base, turn), values in zip(fresh, turned):
                add((base, turn), values)
            words = [(base, turn) for _, base, turn in ahead]
            return words, turned[size - CARRY :]

        def place_many(step, carry):
            last = jnp.logical_and(step == many - 1, few == 0)
            return place(step * UNROLL, UNROLL, last, carry)

        def place_few(step, carry):
            return place(many * UNROLL, UNROLL // 2, True, carry)

        carry = lax.fori_loop(0, many, place_many, carry)
        carry = lax.fori_loop(0, few, place_few, carry)

        @pl.when(c >= 2)
        def _():
            for k in range(DEEP):
                for v in range(TILES):
                    out_copy(c - 2, k, v).wait()

        bank = lax.rem(c, 2)
        ends = []
        for k in range(DEEP):
            for i in range(NY // 32):
                first = c * pitch + (WINDOWS - 1) * NY + 32 * i
                end = accs[k][pl.ds(first, 8, stride=4), :]
                for r in range(1, 4):
                    end = jnp.where(lane >= 32 * r, accs[k][pl.ds(first + r, 8, stride=4), :], end)
                tail[bank * DEEP + k, pl.ds(32 * i, 8, stride=4), :] = end[:, :TAIL]
                ends.append(end)
        end = jnp.concatenate(ends, axis=0)
        high = end.astype(jnp.bfloat16)
        low = (end - high.astype(jnp.float32)).astype(jnp.bfloat16)
        moved = jnp.dot(jnp.concatenate([high, low], axis=1), move, preferred_element_type=jnp.float32)
        for k in range(DEEP):
            for i in range(NY // 32):
                for r in range(1, 4):
                    first = k * (NY // 4) + 8 * i
                    value = moved[first : first + 8, (r - 1) * LANES : (r - 1) * LANES + TAIL]
                    tail[bank * DEEP + k, pl.ds(r + 32 * i, 8, stride=4), :] = value
        for k in range(DEEP):
            for i in range(NY // 32):
                for r in range(4):
                    x_of = lax.bitwise_and(lane - 32 * r, LANES - 1)
                    first = c * pitch + r + 32 * i
                    parts = [accs[k][pl.ds(first + t * NY, 8, stride=4), :] for t in range(WINDOWS)]
                    for v in range(NX // LANES):
                        sum_v = None
                        for t in range(WINDOWS):
                            low = max(STEP * t - LANES * v, 0)
                            high = min(STEP * t + LANES - LANES * v, LANES)
                            if low >= high:
                                continue
                            value = parts[t]
                            if low > 0:
                                value = jnp.where(x_of >= low, value, 0.0)
                            elif high < LANES:
                                value = jnp.where(x_of < high, value, 0.0)
                            sum_v = value if sum_v is None else sum_v + value
                        if r:
                            sum_v = pltpu.roll(sum_v, LANES - 32 * r, 1)
                        stage[bank * DEEP + k, v, pl.ds(r + 32 * i, 8, stride=4), :] = sum_v
            for v in range(TILES):
                out_copy(c, k, v).start()
        return carry

    first = [describe(0, u) for u in range(CARRY)]
    turned = [turned_planes(words) for words in first]
    lax.fori_loop(0, CHUNKS, chunk, ([(base, turn) for _, base, turn in first], turned))
    for c in (CHUNKS - 2, CHUNKS - 1):
        for k in range(DEEP):
            for v in range(TILES):
                out_copy(jnp.int32(c), k, v).wait()


def place_boxes(packed, hot, table, counts, shapes, sums, slots):
    stride = 2 * slots + 1
    vmem = pl.BlockSpec(memory_space=pltpu.VMEM)
    inputs = (packed, hot, table, counts, shapes, *sums)
    return pl.pallas_call(
        functools.partial(place_kernel, slots, stride),
        out_shape=[
            jax.ShapeDtypeStruct((ZS, NY, NX), jnp.float32),
            *[pltpu.VMEM(value.shape, value.dtype) for value in sums],
        ],
        in_specs=[vmem] * len(inputs),
        out_specs=[pl.BlockSpec(memory_space=pltpu.HBM)] + [vmem] * (1 + DEEP),
        input_output_aliases={5 + k: 1 + k for k in range(1 + DEEP)},
        scratch_shapes=[
            pltpu.VMEM((2 * DEEP, NX // LANES, NY, LANES), jnp.float32),
            pltpu.VMEM((2 * DEEP, NY, max(TAIL, 1)), jnp.float32),
            *[pltpu.SMEM((2 * slots,), jnp.int32)] * 3,
            pltpu.SMEM((CHUNKS, LANES), jnp.int32),
            pltpu.SemaphoreType.DMA((4,)),
            pltpu.SemaphoreType.DMA((2 * DEEP, TILES)),
        ],
        compiler_params=pltpu.CompilerParams(vmem_limit_bytes=6 * 1024 * 1024),
    )(*[pltpu.with_memory_space_constraint(value, pltpu.VMEM) for value in inputs])[0]


def share_kernel(
    bands, slabs, coef_ref, occupation_ref, shapes_ref, corners_ref,
    out_ref, hot_ref, table_ref, counts_ref, shp, boxes, *refs,
):
    accs, refs = refs[:DEEP], refs[DEEP:]
    (
    raw, level, spots, plain, part, parts, mine, rows, load_sem, shape_sem, send_a, recv_a, send_b, recv_b,
    ) = refs
    band = lax.axis_index("band")
    slab = lax.axis_index("grid")
    barrier = pltpu.get_barrier_semaphore()
    mesh_id = pl.DeviceIdType.MESH

    def band_peer(d):
        return (lax.rem(band + d, bands), slab)

    def slab_peer(d):
        return (band, lax.rem(slab + d, slabs))

    peers = [band_peer(d) for d in range(1, bands)] + [slab_peer(d) for d in range(1, slabs)]
    for peer in peers:
        pl.semaphore_signal(barrier, inc=1, device_id=peer, device_id_type=mesh_id)
    loads = [
        pltpu.make_async_copy(occupation_ref, level, load_sem.at[0]),
        pltpu.make_async_copy(coef_ref, raw, load_sem.at[1]),
        pltpu.make_async_copy(corners_ref, spots, load_sem.at[2]),
    ]
    for load in loads:
        load.start()
    for load in loads:
        load.wait()
    shape_load = pltpu.make_async_copy(shapes_ref, shp, shape_sem)
    shape_load.start()
    weight = level[...].astype(jnp.float32) * 0.5

    projectors, atoms, depth = raw.shape
    half = atoms // 2
    for i in range(projectors):
        plain[i] = raw[i].astype(jnp.float32)
    lane = lax.broadcasted_iota(jnp.int32, (1, LANES), 1)
    main = jnp.zeros((atoms, LANES), jnp.float32)
    rest = jnp.zeros((half, LANES), jnp.float32)
    pair = 0
    for i in range(projectors):
        left = plain[i] * weight
        for j in range(i, projectors):
            product = left * plain[j]
            total = product[:, :LANES]
            for v in range(1, depth // LANES):
                total = total + product[:, v * LANES : (v + 1) * LANES]
            total = jnp.sum(total, axis=1, keepdims=True)
            if i == j:
                total = total * 0.5
            if pair < LANES:
                main = jnp.where(lane == pair, total, main)
            else:
                rest = jnp.where(lane == pair - LANES, total[:half], rest)
                rest = jnp.where(lane == pair - HALF, total[half:], rest)
            pair = pair + 1
    part[:atoms, :] = main
    part[atoms:, :] = rest
    pl.semaphore_wait(barrier, len(peers))

    copies = []
    for d in range(1, bands):
        copy = pltpu.make_async_remote_copy(
            src_ref=part, dst_ref=parts.at[band], send_sem=send_a.at[d - 1],
            recv_sem=recv_a.at[d - 1], device_id=band_peer(d), device_id_type=mesh_id,
        )
        copy.start()
        copies.append(copy)
    parts[band] = part[...]
    zero = jnp.zeros((64, LANES), jnp.float32)

    def clear(i, carry):
        for acc in accs:
            acc[pl.ds(pl.multiple_of(i * 64, 64), 64), :] = zero
        return carry

    lax.fori_loop(0, accs[0].shape[0] // 64, clear, 0)
    border = PAD * (hot_ref.shape[0] + 1)

    def clear_border(i, carry):
        for edge in (0, boxes.shape[0] - border):
            boxes[pl.ds(pl.multiple_of(edge + i * 32, 8), 32), :] = zero[:32]
        return carry

    lax.fori_loop(0, border // 32, clear_border, 0)
    for copy in copies:
        copy.wait()
    total = parts[0]
    for b in range(1, bands):
        total = total + parts[b]
    packed = total.astype(jnp.bfloat16)
    mine[...] = packed
    copies = []
    for d in range(1, slabs):
        copy = pltpu.make_async_remote_copy(
            src_ref=mine, dst_ref=rows.at[slab], send_sem=send_b.at[d - 1],
            recv_sem=recv_b.at[d - 1], device_id=slab_peer(d), device_id_type=mesh_id,
        )
        copy.start()
        copies.append(copy)
    rows[slab] = packed
    count = hot_ref.shape[0]
    plan_slots(slab, spots, count, count + 1, hot_ref, table_ref, counts_ref)
    for copy in copies:
        copy.wait()
    out_ref[...] = rows[...]
    shape_load.wait()


def share(coefficients, occupation, shapes, corners, bands, slabs):
    atoms, projectors, depth = coefficients.shape
    lines = atoms + atoms // 2
    slots = 4 * atoms
    f32 = jnp.float32
    vmem = pl.BlockSpec(memory_space=pltpu.VMEM)
    hbm = pl.BlockSpec(memory_space=pltpu.HBM)
    inputs = (jnp.transpose(coefficients, (1, 0, 2)), occupation.reshape(1, depth), shapes, corners)
    return pl.pallas_call(
        functools.partial(share_kernel, bands, slabs),
        out_shape=[
            pltpu.VMEM((slabs, lines, LANES), jnp.bfloat16),
            pltpu.VMEM((slots, corners.shape[1]), jnp.bfloat16),
            pltpu.VMEM((8, slots), jnp.int32),
            pltpu.VMEM((CHUNKS, LANES), jnp.int32),
            pltpu.VMEM(shapes.shape, shapes.dtype),
            pltpu.VMEM(((shapes.shape[1] // LANES + 2 * PAD) * (slots + 1), LANES), f32),
            *[pltpu.VMEM((CHUNKS * WINDOWS * NY, LANES), f32)] * DEEP,
        ],
        in_specs=[hbm] * 4,
        out_specs=[vmem] * (6 + DEEP),
        scratch_shapes=[
            pltpu.VMEM((projectors, atoms, depth), jnp.bfloat16),
            pltpu.VMEM((1, depth), jnp.int32),
            pltpu.VMEM(corners.shape, jnp.int32),
            pltpu.VMEM((projectors, atoms, depth), f32),
            pltpu.VMEM((lines, LANES), f32),
            pltpu.VMEM((bands, lines, LANES), f32),
            pltpu.VMEM((lines, LANES), jnp.bfloat16),
            pltpu.VMEM((slabs, lines, LANES), jnp.bfloat16),
            pltpu.SemaphoreType.DMA((3,)),
            pltpu.SemaphoreType.DMA,
            pltpu.SemaphoreType.DMA((bands - 1,)),
            pltpu.SemaphoreType.DMA((bands - 1,)),
            pltpu.SemaphoreType.DMA((slabs - 1,)),
            pltpu.SemaphoreType.DMA((slabs - 1,)),
        ],
        compiler_params=pltpu.CompilerParams(
            collective_id=0, has_side_effects=True, vmem_limit_bytes=6 * 1024 * 1024
        ),
    )(*[pltpu.with_memory_space_constraint(value, pltpu.HBM) for value in inputs])


def body(coefficients, occupation, shapes, corners):
    bands, slabs = lax.axis_size("band"), lax.axis_size("grid")
    packed, hot, table, counts, shapes, *sums = share(
        coefficients, occupation, shapes, corners, bands, slabs
    )
    return place_boxes(packed, hot, table, counts, shapes, sums, 2 * coefficients.shape[0])


def solution(mesh):
    placed = (P("grid", None, "band"), P("band"), P(), P())
    return jax.shard_map(
        body, mesh=mesh, in_specs=placed, out_specs=P("grid", None, None), check_vma=False
    )
```

```python
import functools

import jax
import jax.numpy as jnp
from jax import lax
from jax.experimental import pallas as pl
from jax.experimental.pallas import tpu as pltpu
from jax.sharding import PartitionSpec as P

BOX = 32
ZS = 32
NY = 288
NX = 288
LANES = 128
STEP = LANES - BOX
HALF = LANES // 2


WINDOWS = (NX - BOX) // STEP + 1
TILES = -(-NX // LANES)
TAIL = NX % LANES
DEEP = 4
CHUNKS = ZS // DEEP
PAD = 8 * DEEP
UNROLL = 24
CARRY = 4


def plan_slots(slab, corners_ref, count, stride, hot_ref, table_ref, counts_ref):
    atoms = corners_ref.shape[1]

    depth = corners_ref[0:1, :]
    owner = lax.shift_right_logical(depth, ZS.bit_length() - 1)
    local = depth - owner * ZS
    own = owner == slab
    below = jnp.logical_and(owner == slab - 1, local > 0)
    index = lax.broadcasted_iota(jnp.int32, (1, atoms), 1)
    key = jnp.where(own, local, jnp.where(below, ZS + 1 + local, ZS)) * atoms + index
    key = key.astype(jnp.float32)
    slot_rows = []
    for a in range(atoms // LANES):
        mine = key[:, a * LANES : (a + 1) * LANES]
        rank = jnp.zeros((1, LANES), jnp.float32)
        for b in range(atoms // LANES):
            other = jnp.broadcast_to(key[:, b * LANES : (b + 1) * LANES], (LANES, LANES)).T
            rank = rank + jnp.sum((other < mine).astype(jnp.float32), axis=0, keepdims=True)
        slot_rows.append(rank)
    slot_of = jnp.concatenate(slot_rows, axis=1).astype(jnp.int32)
    slot_of = jnp.where(own, slot_of, jnp.where(below, slot_of + (count - atoms), -1))
    hot = lax.broadcasted_iota(jnp.int32, (count, atoms), 0) == slot_of
    hot = hot.astype(jnp.float32).astype(jnp.bfloat16)
    hot_ref[...] = hot
    start = jnp.where(own, -local, ZS - local)
    line = lax.broadcasted_iota(jnp.int32, (8, atoms), 0)
    traits = jnp.where(line == 0, corners_ref[1:2, :], jnp.where(line == 1, corners_ref[2:3, :], start))
    traits = traits.astype(jnp.float32).astype(jnp.bfloat16)
    traits = lax.dot_general(traits, hot, (((1,), (1,)), ((), ())), preferred_element_type=jnp.float32)
    traits = traits.astype(jnp.int32)
    row, column, start = traits[0:1, :], traits[1:2, :], traits[2:3, :]
    window = jnp.zeros_like(column)
    for t in range(1, WINDOWS):
        window = window + (column >= t * STEP).astype(jnp.int32)
    source = (PAD + start * 8) * stride + lax.broadcasted_iota(jnp.int32, (1, count), 1)
    target = window * NY + row
    turn = lax.bitwise_and(column + 32 * row, LANES - 1)
    for at, value in enumerate((source, target, turn)):
        table_ref[at : at + 1, :] = value
    bound = lax.broadcasted_iota(jnp.int32, (CHUNKS, atoms), 0) * DEEP
    near = jnp.sum(jnp.where(jnp.logical_and(own, local < bound + DEEP), 1.0, 0.0), axis=1, keepdims=True)
    far = jnp.sum(jnp.where(jnp.logical_and(below, local > bound), 1.0, 0.0), axis=1, keepdims=True)
    side = lax.broadcasted_iota(jnp.int32, (CHUNKS, LANES), 1)
    counts_ref[...] = jnp.where(side == 0, near, far).astype(jnp.int32)


def place_kernel(
    slots, stride, packed_ref, hot_ref, table_ref, counts_ref, shapes_ref, *refs,
):
    out_ref = refs[DEEP + 1]
    boxes, *accs = refs[DEEP + 2 : 2 * DEEP + 3]
    stage, tail, sources, targets, turns, sizes, word_sem, out_sem = refs[2 * DEEP + 3 :]
    columns = shapes_ref.shape[1]
    count = 2 * slots
    atoms = hot_ref.shape[1]
    hot = hot_ref[...]
    word_copies = [
        pltpu.make_async_copy(table_ref.at[0], sources, word_sem.at[0]),
        pltpu.make_async_copy(table_ref.at[1], targets, word_sem.at[1]),
        pltpu.make_async_copy(table_ref.at[2], turns, word_sem.at[2]),
        pltpu.make_async_copy(counts_ref, sizes, word_sem.at[3]),
    ]
    for copy in word_copies:
        copy.start()

    slabs, lines, _ = packed_ref.shape
    share = lines * 2 // 3
    firsts, rests = [], []
    for s in range(slabs):
        firsts.append(packed_ref[s, :share, :])
        rests.extend([packed_ref[s, share:, :]] * 2)
    lane = lax.broadcasted_iota(jnp.int32, (atoms, LANES), 1)
    side = lax.rem(lax.broadcasted_iota(jnp.int32, (atoms, LANES), 0), share) >= share // 2
    rest = jnp.concatenate(rests, axis=0).astype(jnp.float32)
    rest = jnp.where(lane == LANES - 1, side.astype(jnp.float32), rest).astype(jnp.bfloat16)
    first = jnp.dot(hot, jnp.concatenate(firsts, axis=0), preferred_element_type=jnp.float32)
    rest = jnp.dot(hot, rest, preferred_element_type=jnp.float32)
    rest = jnp.where(rest[:, LANES - 1 :] > 0.5, pltpu.roll(rest, HALF, 1), rest)
    pairs = shapes_ref.shape[0]
    rows = jnp.concatenate([first, rest[:, : pairs - LANES]], axis=1).astype(jnp.bfloat16)

    span = 32768

    def multiply(s, carry):
        at = pl.multiple_of(s * span, span)
        for part in range(span // 1024):
            product = jnp.dot(
                rows, shapes_ref[:, pl.ds(at + part * 1024, 1024)], preferred_element_type=jnp.float32
            )
            for c in range(1024 // LANES):
                spot = (PAD + at // LANES + part * 1024 // LANES + c) * stride
                boxes[pl.ds(spot, count), :] = product[:, c * LANES : (c + 1) * LANES]
        return carry

    lax.fori_loop(0, columns // span, multiply, 0)
    for copy in word_copies:
        copy.wait()

    lane = lax.broadcasted_iota(jnp.int32, (8, LANES), 1)
    pitch = WINDOWS * NY
    come = lax.bitwise_and(lax.broadcasted_iota(jnp.int32, (2 * LANES, 3 * LANES), 0), LANES - 1)
    goes = lax.broadcasted_iota(jnp.int32, (2 * LANES, 3 * LANES), 1)
    goes = lax.bitwise_and(goes, LANES - 1) + 32 * (lax.shift_right_logical(goes, 7) + 1)
    move = jnp.where(come == goes, 1.0, 0.0).astype(jnp.bfloat16)

    def out_copy(c, k, v):
        width = min(LANES, NX - v * LANES)
        slot = lax.rem(c, 2) * DEEP + k
        return pltpu.make_async_copy(
            stage.at[slot, v] if width == LANES else tail.at[slot],
            out_ref.at[c * DEEP + k, :, pl.ds(v * LANES, width)],
            out_sem.at[slot, v],
        )

    def describe(c, item):
        far = sizes[c, 1]
        slot = lax.bitwise_and(item - far, count - 1)
        filled = item < sizes[c, 0] + far
        source = jnp.where(filled, sources[slot] + c * (DEEP * 8 * stride), 0)
        return source, targets[slot] + c * pitch, turns[slot]

    def turned_planes(words):
        source, _, turn = words
        planes = [boxes[pl.ds(source + k * 8 * stride, 8, stride=stride), :] for k in range(DEEP)]
        return [pltpu.roll(plane, turn, 1) for plane in planes]

    def chunk(c, carry):
        total = sizes[c, 0] + sizes[c, 1]
        halves = jnp.maximum((total + UNROLL // 2 - 1) // (UNROLL // 2), 1)
        many = lax.shift_right_logical(halves, 1)
        few = lax.bitwise_and(halves, 1)

        def add(words, values):
            base, turn = words
            part = lax.shift_right_logical(lax.bitwise_and(lane - turn, LANES - 1), 5)
            masks = [jnp.where(part == g, 1.0, 0.0) for g in range(4)]
            for g in range(4):
                for k in range(DEEP):
                    at = pl.ds(base + g, 8, stride=4)
                    accs[k][at, :] = accs[k][at, :] + masks[g] * values[k]

        def place(begin, size, last, carry):
            after = jnp.where(last, jnp.minimum(c + 1, CHUNKS - 1), c)
            fresh = [describe(c, begin + u) for u in range(CARRY, size)]
            ahead = [describe(after, jnp.where(last, 0, begin + size) + u) for u in range(CARRY)]
            turned = [turned_planes(words) for words in fresh + ahead]
            for words, values in zip(carry[0], carry[1]):
                add(words, values)
            for (_, base, turn), values in zip(fresh, turned):
                add((base, turn), values)
            words = [(base, turn) for _, base, turn in ahead]
            return words, turned[size - CARRY :]

        def place_many(step, carry):
            last = jnp.logical_and(step == many - 1, few == 0)
            return place(step * UNROLL, UNROLL, last, carry)

        def place_few(step, carry):
            return place(many * UNROLL, UNROLL // 2, True, carry)

        carry = lax.fori_loop(0, many, place_many, carry)
        carry = lax.fori_loop(0, few, place_few, carry)

        @pl.when(c >= 2)
        def _():
            for k in range(DEEP):
                for v in range(TILES):
                    out_copy(c - 2, k, v).wait()

        bank = lax.rem(c, 2)
        ends = []
        for k in range(DEEP):
            for i in range(NY // 32):
                first = c * pitch + (WINDOWS - 1) * NY + 32 * i
                end = accs[k][pl.ds(first, 8, stride=4), :]
                for r in range(1, 4):
                    end = jnp.where(lane >= 32 * r, accs[k][pl.ds(first + r, 8, stride=4), :], end)
                tail[bank * DEEP + k, pl.ds(32 * i, 8, stride=4), :] = end[:, :TAIL]
                ends.append(end)
        end = jnp.concatenate(ends, axis=0)
        high = end.astype(jnp.bfloat16)
        low = (end - high.astype(jnp.float32)).astype(jnp.bfloat16)
        moved = jnp.dot(jnp.concatenate([high, low], axis=1), move, preferred_element_type=jnp.float32)
        for k in range(DEEP):
            for i in range(NY // 32):
                for r in range(1, 4):
                    first = k * (NY // 4) + 8 * i
                    value = moved[first : first + 8, (r - 1) * LANES : (r - 1) * LANES + TAIL]
                    tail[bank * DEEP + k, pl.ds(r + 32 * i, 8, stride=4), :] = value
        for k in range(DEEP):
            for i in range(NY // 32):
                for r in range(4):
                    x_of = lax.bitwise_and(lane - 32 * r, LANES - 1)
                    first = c * pitch + r + 32 * i
                    parts = [accs[k][pl.ds(first + t * NY, 8, stride=4), :] for t in range(WINDOWS)]
                    for v in range(NX // LANES):
                        sum_v = None
                        for t in range(WINDOWS):
                            low = max(STEP * t - LANES * v, 0)
                            high = min(STEP * t + LANES - LANES * v, LANES)
                            if low >= high:
                                continue
                            value = parts[t]
                            if low > 0:
                                value = jnp.where(x_of >= low, value, 0.0)
                            elif high < LANES:
                                value = jnp.where(x_of < high, value, 0.0)
                            sum_v = value if sum_v is None else sum_v + value
                        if r:
                            sum_v = pltpu.roll(sum_v, LANES - 32 * r, 1)
                        stage[bank * DEEP + k, v, pl.ds(r + 32 * i, 8, stride=4), :] = sum_v
            for v in range(TILES):
                out_copy(c, k, v).start()
        return carry

    first = [describe(0, u) for u in range(CARRY)]
    turned = [turned_planes(words) for words in first]
    lax.fori_loop(0, CHUNKS, chunk, ([(base, turn) for _, base, turn in first], turned))
    for c in (CHUNKS - 2, CHUNKS - 1):
        for k in range(DEEP):
            for v in range(TILES):
                out_copy(jnp.int32(c), k, v).wait()


def place_boxes(packed, hot, table, counts, shapes, sums, slots):
    stride = 2 * slots + 1
    vmem = pl.BlockSpec(memory_space=pltpu.VMEM)
    inputs = (packed, hot, table, counts, shapes, *sums)
    return pl.pallas_call(
        functools.partial(place_kernel, slots, stride),
        out_shape=[
            jax.ShapeDtypeStruct((ZS, NY, NX), jnp.float32),
            *[pltpu.VMEM(value.shape, value.dtype) for value in sums],
        ],
        in_specs=[vmem] * len(inputs),
        out_specs=[pl.BlockSpec(memory_space=pltpu.HBM)] + [vmem] * (1 + DEEP),
        input_output_aliases={5 + k: 1 + k for k in range(1 + DEEP)},
        scratch_shapes=[
            pltpu.VMEM((2 * DEEP, NX // LANES, NY, LANES), jnp.float32),
            pltpu.VMEM((2 * DEEP, NY, max(TAIL, 1)), jnp.float32),
            *[pltpu.SMEM((2 * slots,), jnp.int32)] * 3,
            pltpu.SMEM((CHUNKS, LANES), jnp.int32),
            pltpu.SemaphoreType.DMA((4,)),
            pltpu.SemaphoreType.DMA((2 * DEEP, TILES)),
        ],
        compiler_params=pltpu.CompilerParams(vmem_limit_bytes=6 * 1024 * 1024),
    )(*[pltpu.with_memory_space_constraint(value, pltpu.VMEM) for value in inputs])[0]


def share_kernel(
    bands, slabs, coef_ref, occupation_ref, shapes_ref, corners_ref,
    out_ref, hot_ref, table_ref, counts_ref, shp, boxes, *refs,
):
    accs, refs = refs[:DEEP], refs[DEEP:]
    (
    raw, level, spots, plain, part, parts, mine, rows, load_sem, shape_sem, send_a, recv_a, send_b, recv_b,
    ) = refs
    band = lax.axis_index("band")
    slab = lax.axis_index("grid")
    barrier = pltpu.get_barrier_semaphore()
    mesh_id = pl.DeviceIdType.MESH

    def band_peer(d):
        return (lax.rem(band + d, bands), slab)

    def slab_peer(d):
        return (band, lax.rem(slab + d, slabs))

    peers = [band_peer(d) for d in range(1, bands)] + [slab_peer(d) for d in range(1, slabs)]
    for peer in peers:
        pl.semaphore_signal(barrier, inc=1, device_id=peer, device_id_type=mesh_id)
    loads = [
        pltpu.make_async_copy(occupation_ref, level, load_sem.at[0]),
        pltpu.make_async_copy(coef_ref, raw, load_sem.at[1]),
        pltpu.make_async_copy(corners_ref, spots, load_sem.at[2]),
    ]
    for load in loads:
        load.start()
    for load in loads:
        load.wait()
    shape_load = pltpu.make_async_copy(shapes_ref, shp, shape_sem)
    shape_load.start()
    weight = level[...].astype(jnp.float32) * 0.5

    projectors, atoms, depth = raw.shape
    half = atoms // 2
    for i in range(projectors):
        plain[i] = raw[i].astype(jnp.float32)
    lane = lax.broadcasted_iota(jnp.int32, (1, LANES), 1)
    main = jnp.zeros((atoms, LANES), jnp.float32)
    rest = jnp.zeros((half, LANES), jnp.float32)
    pair = 0
    for i in range(projectors):
        left = plain[i] * weight
        for j in range(i, projectors):
            product = left * plain[j]
            total = product[:, :LANES]
            for v in range(1, depth // LANES):
                total = total + product[:, v * LANES : (v + 1) * LANES]
            total = jnp.sum(total, axis=1, keepdims=True)
            if i == j:
                total = total * 0.5
            if pair < LANES:
                main = jnp.where(lane == pair, total, main)
            else:
                rest = jnp.where(lane == pair - LANES, total[:half], rest)
                rest = jnp.where(lane == pair - HALF, total[half:], rest)
            pair = pair + 1
    part[:atoms, :] = main
    part[atoms:, :] = rest
    pl.semaphore_wait(barrier, len(peers))

    copies = []
    for d in range(1, bands):
        copy = pltpu.make_async_remote_copy(
            src_ref=part, dst_ref=parts.at[band], send_sem=send_a.at[d - 1],
            recv_sem=recv_a.at[d - 1], device_id=band_peer(d), device_id_type=mesh_id,
        )
        copy.start()
        copies.append(copy)
    parts[band] = part[...]
    zero = jnp.zeros((64, LANES), jnp.float32)

    def clear(i, carry):
        for acc in accs:
            acc[pl.ds(pl.multiple_of(i * 64, 64), 64), :] = zero
        return carry

    lax.fori_loop(0, accs[0].shape[0] // 64, clear, 0)
    border = PAD * (hot_ref.shape[0] + 1)

    def clear_border(i, carry):
        for edge in (0, boxes.shape[0] - border):
            boxes[pl.ds(pl.multiple_of(edge + i * 32, 8), 32), :] = zero[:32]
        return carry

    lax.fori_loop(0, border // 32, clear_border, 0)
    for copy in copies:
        copy.wait()
    total = parts[0]
    for b in range(1, bands):
        total = total + parts[b]
    packed = total.astype(jnp.bfloat16)
    mine[...] = packed
    copies = []
    for d in range(1, slabs):
        copy = pltpu.make_async_remote_copy(
            src_ref=mine, dst_ref=rows.at[slab], send_sem=send_b.at[d - 1],
            recv_sem=recv_b.at[d - 1], device_id=slab_peer(d), device_id_type=mesh_id,
        )
        copy.start()
        copies.append(copy)
    rows[slab] = packed
    count = hot_ref.shape[0]
    plan_slots(slab, spots, count, count + 1, hot_ref, table_ref, counts_ref)
    for copy in copies:
        copy.wait()
    out_ref[...] = rows[...]
    shape_load.wait()


def share(coefficients, occupation, shapes, corners, bands, slabs):
    atoms, projectors, depth = coefficients.shape
    lines = atoms + atoms // 2
    slots = 4 * atoms
    f32 = jnp.float32
    vmem = pl.BlockSpec(memory_space=pltpu.VMEM)
    hbm = pl.BlockSpec(memory_space=pltpu.HBM)
    inputs = (jnp.transpose(coefficients, (1, 0, 2)), occupation.reshape(1, depth), shapes, corners)
    return pl.pallas_call(
        functools.partial(share_kernel, bands, slabs),
        out_shape=[
            pltpu.VMEM((slabs, lines, LANES), jnp.bfloat16),
            pltpu.VMEM((slots, corners.shape[1]), jnp.bfloat16),
            pltpu.VMEM((8, slots), jnp.int32),
            pltpu.VMEM((CHUNKS, LANES), jnp.int32),
            pltpu.VMEM(shapes.shape, shapes.dtype),
            pltpu.VMEM(((shapes.shape[1] // LANES + 2 * PAD) * (slots + 1), LANES), f32),
            *[pltpu.VMEM((CHUNKS * WINDOWS * NY, LANES), f32)] * DEEP,
        ],
        in_specs=[hbm] * 4,
        out_specs=[vmem] * (6 + DEEP),
        scratch_shapes=[
            pltpu.VMEM((projectors, atoms, depth), jnp.bfloat16),
            pltpu.VMEM((1, depth), jnp.int32),
            pltpu.VMEM(corners.shape, jnp.int32),
            pltpu.VMEM((projectors, atoms, depth), f32),
            pltpu.VMEM((lines, LANES), f32),
            pltpu.VMEM((bands, lines, LANES), f32),
            pltpu.VMEM((lines, LANES), jnp.bfloat16),
            pltpu.VMEM((slabs, lines, LANES), jnp.bfloat16),
            pltpu.SemaphoreType.DMA((3,)),
            pltpu.SemaphoreType.DMA,
            pltpu.SemaphoreType.DMA((bands - 1,)),
            pltpu.SemaphoreType.DMA((bands - 1,)),
            pltpu.SemaphoreType.DMA((slabs - 1,)),
            pltpu.SemaphoreType.DMA((slabs - 1,)),
        ],
        compiler_params=pltpu.CompilerParams(
            collective_id=0, has_side_effects=True, vmem_limit_bytes=6 * 1024 * 1024
        ),
    )(*[pltpu.with_memory_space_constraint(value, pltpu.HBM) for value in inputs])


def body(coefficients, occupation, shapes, corners):
    bands, slabs = lax.axis_size("band"), lax.axis_size("grid")
    packed, hot, table, counts, shapes, *sums = share(
        coefficients, occupation, shapes, corners, bands, slabs
    )
    return place_boxes(packed, hot, table, counts, shapes, sums, 2 * coefficients.shape[0])


def solution(mesh):
    placed = (P("grid", None, "band"), P("band"), P(), P())
    return jax.shard_map(
        body, mesh=mesh, in_specs=placed, out_specs=P("grid", None, None), check_vma=False
    )
```

```python
import functools

import jax
import jax.numpy as jnp
from jax import lax
from jax.experimental import pallas as pl
from jax.experimental.pallas import tpu as pltpu
from jax.sharding import PartitionSpec as P

BOX = 32
ZS = 32
NY = 288
NX = 288
LANES = 128
STEP = LANES - BOX
HALF = LANES // 2


WINDOWS = (NX - BOX) // STEP + 1
TILES = -(-NX // LANES)
TAIL = NX % LANES
DEEP = 4
CHUNKS = ZS // DEEP
PAD = 8 * DEEP
UNROLL = 24
CARRY = 4


def plan_slots(slab, corners_ref, count, stride, hot_ref, table_ref, counts_ref):
    atoms = corners_ref.shape[1]

    depth = corners_ref[0:1, :]
    owner = lax.shift_right_logical(depth, ZS.bit_length() - 1)
    local = depth - owner * ZS
    own = owner == slab
    below = jnp.logical_and(owner == slab - 1, local > 0)
    index = lax.broadcasted_iota(jnp.int32, (1, atoms), 1)
    key = jnp.where(own, local, jnp.where(below, ZS + 1 + local, ZS)) * atoms + index
    key = key.astype(jnp.float32)
    slot_rows = []
    for a in range(atoms // LANES):
        mine = key[:, a * LANES : (a + 1) * LANES]
        rank = jnp.zeros((1, LANES), jnp.float32)
        for b in range(atoms // LANES):
            other = jnp.broadcast_to(key[:, b * LANES : (b + 1) * LANES], (LANES, LANES)).T
            rank = rank + jnp.sum((other < mine).astype(jnp.float32), axis=0, keepdims=True)
        slot_rows.append(rank)
    slot_of = jnp.concatenate(slot_rows, axis=1).astype(jnp.int32)
    slot_of = jnp.where(own, slot_of, jnp.where(below, slot_of + (count - atoms), -1))
    hot = lax.broadcasted_iota(jnp.int32, (count, atoms), 0) == slot_of
    hot = hot.astype(jnp.float32).astype(jnp.bfloat16)
    hot_ref[...] = hot
    start = jnp.where(own, -local, ZS - local)
    line = lax.broadcasted_iota(jnp.int32, (8, atoms), 0)
    traits = jnp.where(line == 0, corners_ref[1:2, :], jnp.where(line == 1, corners_ref[2:3, :], start))
    traits = traits.astype(jnp.float32).astype(jnp.bfloat16)
    traits = lax.dot_general(traits, hot, (((1,), (1,)), ((), ())), preferred_element_type=jnp.float32)
    traits = traits.astype(jnp.int32)
    row, column, start = traits[0:1, :], traits[1:2, :], traits[2:3, :]
    window = jnp.zeros_like(column)
    for t in range(1, WINDOWS):
        window = window + (column >= t * STEP).astype(jnp.int32)
    source = (PAD + start * 8) * stride + lax.broadcasted_iota(jnp.int32, (1, count), 1)
    target = window * NY + row
    turn = lax.bitwise_and(column + 32 * row, LANES - 1)
    for at, value in enumerate((source, target, turn)):
        table_ref[at : at + 1, :] = value
    bound = lax.broadcasted_iota(jnp.int32, (CHUNKS, atoms), 0) * DEEP
    near = jnp.sum(jnp.where(jnp.logical_and(own, local < bound + DEEP), 1.0, 0.0), axis=1, keepdims=True)
    far = jnp.sum(jnp.where(jnp.logical_and(below, local > bound), 1.0, 0.0), axis=1, keepdims=True)
    side = lax.broadcasted_iota(jnp.int32, (CHUNKS, LANES), 1)
    counts_ref[...] = jnp.where(side == 0, near, far).astype(jnp.int32)


def place_kernel(
    slots, stride, packed_ref, hot_ref, table_ref, counts_ref, shapes_ref, *refs,
):
    out_ref = refs[DEEP + 1]
    boxes, *accs = refs[DEEP + 2 : 2 * DEEP + 3]
    stage, tail, sources, targets, turns, sizes, word_sem, out_sem = refs[2 * DEEP + 3 :]
    columns = shapes_ref.shape[1]
    count = 2 * slots
    atoms = hot_ref.shape[1]
    hot = hot_ref[...]
    word_copies = [
        pltpu.make_async_copy(table_ref.at[0], sources, word_sem.at[0]),
        pltpu.make_async_copy(table_ref.at[1], targets, word_sem.at[1]),
        pltpu.make_async_copy(table_ref.at[2], turns, word_sem.at[2]),
        pltpu.make_async_copy(counts_ref, sizes, word_sem.at[3]),
    ]
    for copy in word_copies:
        copy.start()

    slabs, lines, _ = packed_ref.shape
    share = lines * 2 // 3
    firsts, rests = [], []
    for s in range(slabs):
        firsts.append(packed_ref[s, :share, :])
        rests.extend([packed_ref[s, share:, :]] * 2)
    lane = lax.broadcasted_iota(jnp.int32, (atoms, LANES), 1)
    side = lax.rem(lax.broadcasted_iota(jnp.int32, (atoms, LANES), 0), share) >= share // 2
    rest = jnp.concatenate(rests, axis=0).astype(jnp.float32)
    rest = jnp.where(lane == LANES - 1, side.astype(jnp.float32), rest).astype(jnp.bfloat16)
    first = jnp.dot(hot, jnp.concatenate(firsts, axis=0), preferred_element_type=jnp.float32)
    rest = jnp.dot(hot, rest, preferred_element_type=jnp.float32)
    rest = jnp.where(rest[:, LANES - 1 :] > 0.5, pltpu.roll(rest, HALF, 1), rest)
    pairs = shapes_ref.shape[0]
    rows = jnp.concatenate([first, rest[:, : pairs - LANES]], axis=1).astype(jnp.bfloat16)

    span = 32768

    def multiply(s, carry):
        at = pl.multiple_of(s * span, span)
        for part in range(span // 1024):
            product = jnp.dot(
                rows, shapes_ref[:, pl.ds(at + part * 1024, 1024)], preferred_element_type=jnp.float32
            )
            for c in range(1024 // LANES):
                spot = (PAD + at // LANES + part * 1024 // LANES + c) * stride
                boxes[pl.ds(spot, count), :] = product[:, c * LANES : (c + 1) * LANES]
        return carry

    lax.fori_loop(0, columns // span, multiply, 0)
    for copy in word_copies:
        copy.wait()

    lane = lax.broadcasted_iota(jnp.int32, (8, LANES), 1)
    pitch = WINDOWS * NY
    come = lax.bitwise_and(lax.broadcasted_iota(jnp.int32, (2 * LANES, 3 * LANES), 0), LANES - 1)
    goes = lax.broadcasted_iota(jnp.int32, (2 * LANES, 3 * LANES), 1)
    goes = lax.bitwise_and(goes, LANES - 1) + 32 * (lax.shift_right_logical(goes, 7) + 1)
    move = jnp.where(come == goes, 1.0, 0.0).astype(jnp.bfloat16)

    def out_copy(c, k, v):
        width = min(LANES, NX - v * LANES)
        slot = lax.rem(c, 2) * DEEP + k
        return pltpu.make_async_copy(
            stage.at[slot, v] if width == LANES else tail.at[slot],
            out_ref.at[c * DEEP + k, :, pl.ds(v * LANES, width)],
            out_sem.at[slot, v],
        )

    def describe(c, item):
        far = sizes[c, 1]
        slot = lax.bitwise_and(item - far, count - 1)
        filled = item < sizes[c, 0] + far
        source = jnp.where(filled, sources[slot] + c * (DEEP * 8 * stride), 0)
        return source, targets[slot] + c * pitch, turns[slot]

    def turned_planes(words):
        source, _, turn = words
        planes = [boxes[pl.ds(source + k * 8 * stride, 8, stride=stride), :] for k in range(DEEP)]
        return [pltpu.roll(plane, turn, 1) for plane in planes]

    def chunk(c, carry):
        total = sizes[c, 0] + sizes[c, 1]
        halves = jnp.maximum((total + UNROLL // 2 - 1) // (UNROLL // 2), 1)
        many = lax.shift_right_logical(halves, 1)
        few = lax.bitwise_and(halves, 1)

        def add(words, values):
            base, turn = words
            part = lax.shift_right_logical(lax.bitwise_and(lane - turn, LANES - 1), 5)
            masks = [jnp.where(part == g, 1.0, 0.0) for g in range(4)]
            for g in range(4):
                for k in range(DEEP):
                    at = pl.ds(base + g, 8, stride=4)
                    accs[k][at, :] = accs[k][at, :] + masks[g] * values[k]

        def place(begin, size, last, carry):
            after = jnp.where(last, jnp.minimum(c + 1, CHUNKS - 1), c)
            fresh = [describe(c, begin + u) for u in range(CARRY, size)]
            ahead = [describe(after, jnp.where(last, 0, begin + size) + u) for u in range(CARRY)]
            turned = [turned_planes(words) for words in fresh + ahead]
            for words, values in zip(carry[0], carry[1]):
                add(words, values)
            for (_, base, turn), values in zip(fresh, turned):
                add((base, turn), values)
            words = [(base, turn) for _, base, turn in ahead]
            return words, turned[size - CARRY :]

        def place_many(step, carry):
            last = jnp.logical_and(step == many - 1, few == 0)
            return place(step * UNROLL, UNROLL, last, carry)

        def place_few(step, carry):
            return place(many * UNROLL, UNROLL // 2, True, carry)

        carry = lax.fori_loop(0, many, place_many, carry)
        carry = lax.fori_loop(0, few, place_few, carry)

        @pl.when(c >= 2)
        def _():
            for k in range(DEEP):
                for v in range(TILES):
                    out_copy(c - 2, k, v).wait()

        bank = lax.rem(c, 2)
        ends = []
        for k in range(DEEP):
            for i in range(NY // 32):
                first = c * pitch + (WINDOWS - 1) * NY + 32 * i
                end = accs[k][pl.ds(first, 8, stride=4), :]
                for r in range(1, 4):
                    end = jnp.where(lane >= 32 * r, accs[k][pl.ds(first + r, 8, stride=4), :], end)
                tail[bank * DEEP + k, pl.ds(32 * i, 8, stride=4), :] = end[:, :TAIL]
                ends.append(end)
        end = jnp.concatenate(ends, axis=0)
        high = end.astype(jnp.bfloat16)
        low = (end - high.astype(jnp.float32)).astype(jnp.bfloat16)
        moved = jnp.dot(jnp.concatenate([high, low], axis=1), move, preferred_element_type=jnp.float32)
        for k in range(DEEP):
            for i in range(NY // 32):
                for r in range(1, 4):
                    first = k * (NY // 4) + 8 * i
                    value = moved[first : first + 8, (r - 1) * LANES : (r - 1) * LANES + TAIL]
                    tail[bank * DEEP + k, pl.ds(r + 32 * i, 8, stride=4), :] = value
        for k in range(DEEP):
            for i in range(NY // 32):
                for r in range(4):
                    x_of = lax.bitwise_and(lane - 32 * r, LANES - 1)
                    first = c * pitch + r + 32 * i
                    parts = [accs[k][pl.ds(first + t * NY, 8, stride=4), :] for t in range(WINDOWS)]
                    for v in range(NX // LANES):
                        sum_v = None
                        for t in range(WINDOWS):
                            low = max(STEP * t - LANES * v, 0)
                            high = min(STEP * t + LANES - LANES * v, LANES)
                            if low >= high:
                                continue
                            value = parts[t]
                            if low > 0:
                                value = jnp.where(x_of >= low, value, 0.0)
                            elif high < LANES:
                                value = jnp.where(x_of < high, value, 0.0)
                            sum_v = value if sum_v is None else sum_v + value
                        if r:
                            sum_v = pltpu.roll(sum_v, LANES - 32 * r, 1)
                        stage[bank * DEEP + k, v, pl.ds(r + 32 * i, 8, stride=4), :] = sum_v
            for v in range(TILES):
                out_copy(c, k, v).start()
        return carry

    first = [describe(0, u) for u in range(CARRY)]
    turned = [turned_planes(words) for words in first]
    lax.fori_loop(0, CHUNKS, chunk, ([(base, turn) for _, base, turn in first], turned))
    for c in (CHUNKS - 2, CHUNKS - 1):
        for k in range(DEEP):
            for v in range(TILES):
                out_copy(jnp.int32(c), k, v).wait()


def place_boxes(packed, hot, table, counts, shapes, sums, slots):
    stride = 2 * slots + 1
    vmem = pl.BlockSpec(memory_space=pltpu.VMEM)
    inputs = (packed, hot, table, counts, shapes, *sums)
    return pl.pallas_call(
        functools.partial(place_kernel, slots, stride),
        out_shape=[
            jax.ShapeDtypeStruct((ZS, NY, NX), jnp.float32),
            *[pltpu.VMEM(value.shape, value.dtype) for value in sums],
        ],
        in_specs=[vmem] * len(inputs),
        out_specs=[pl.BlockSpec(memory_space=pltpu.HBM)] + [vmem] * (1 + DEEP),
        input_output_aliases={5 + k: 1 + k for k in range(1 + DEEP)},
        scratch_shapes=[
            pltpu.VMEM((2 * DEEP, NX // LANES, NY, LANES), jnp.float32),
            pltpu.VMEM((2 * DEEP, NY, max(TAIL, 1)), jnp.float32),
            *[pltpu.SMEM((2 * slots,), jnp.int32)] * 3,
            pltpu.SMEM((CHUNKS, LANES), jnp.int32),
            pltpu.SemaphoreType.DMA((4,)),
            pltpu.SemaphoreType.DMA((2 * DEEP, TILES)),
        ],
        compiler_params=pltpu.CompilerParams(vmem_limit_bytes=6 * 1024 * 1024),
    )(*[pltpu.with_memory_space_constraint(value, pltpu.VMEM) for value in inputs])[0]


def share_kernel(
    bands, slabs, coef_ref, occupation_ref, shapes_ref, corners_ref,
    out_ref, hot_ref, table_ref, counts_ref, shp, boxes, *refs,
):
    accs, refs = refs[:DEEP], refs[DEEP:]
    (
    raw, level, spots, plain, part, parts, mine, rows, load_sem, shape_sem, send_a, recv_a, send_b, recv_b,
    ) = refs
    band = lax.axis_index("band")
    slab = lax.axis_index("grid")
    barrier = pltpu.get_barrier_semaphore()
    mesh_id = pl.DeviceIdType.MESH

    def band_peer(d):
        return (lax.rem(band + d, bands), slab)

    def slab_peer(d):
        return (band, lax.rem(slab + d, slabs))

    peers = [band_peer(d) for d in range(1, bands)] + [slab_peer(d) for d in range(1, slabs)]
    for peer in peers:
        pl.semaphore_signal(barrier, inc=1, device_id=peer, device_id_type=mesh_id)
    loads = [
        pltpu.make_async_copy(occupation_ref, level, load_sem.at[0]),
        pltpu.make_async_copy(coef_ref, raw, load_sem.at[1]),
        pltpu.make_async_copy(corners_ref, spots, load_sem.at[2]),
    ]
    for load in loads:
        load.start()
    for load in loads:
        load.wait()
    shape_load = pltpu.make_async_copy(shapes_ref, shp, shape_sem)
    shape_load.start()
    weight = level[...].astype(jnp.float32) * 0.5

    projectors, atoms, depth = raw.shape
    half = atoms // 2
    for i in range(projectors):
        plain[i] = raw[i].astype(jnp.float32)
    part[...] = jnp.zeros(part.shape, jnp.float32)
    pair = 0
    for i in range(projectors):
        left = plain[i] * weight
        for j in range(i, projectors):
            product = left * plain[j]
            total = product[:, :LANES]
            for v in range(1, depth // LANES):
                total = total + product[:, v * LANES : (v + 1) * LANES]
            total = jnp.sum(total, axis=1, keepdims=True)
            if i == j:
                total = total * 0.5
            if pair < LANES:
                part[:atoms, pair : pair + 1] = total
            else:
                part[atoms:, pair - LANES : pair - LANES + 1] = total[:half]
                part[atoms:, pair - HALF : pair - HALF + 1] = total[half:]
            pair = pair + 1
    pl.semaphore_wait(barrier, len(peers))

    copies = []
    for d in range(1, bands):
        copy = pltpu.make_async_remote_copy(
            src_ref=part, dst_ref=parts.at[band], send_sem=send_a.at[d - 1],
            recv_sem=recv_a.at[d - 1], device_id=band_peer(d), device_id_type=mesh_id,
        )
        copy.start()
        copies.append(copy)
    parts[band] = part[...]
    zero = jnp.zeros((64, LANES), jnp.float32)

    def clear(i, carry):
        for acc in accs:
            acc[pl.ds(pl.multiple_of(i * 64, 64), 64), :] = zero
        return carry

    lax.fori_loop(0, accs[0].shape[0] // 64, clear, 0)
    border = PAD * (hot_ref.shape[0] + 1)

    def clear_border(i, carry):
        for edge in (0, boxes.shape[0] - border):
            boxes[pl.ds(pl.multiple_of(edge + i * 32, 8), 32), :] = zero[:32]
        return carry

    lax.fori_loop(0, border // 32, clear_border, 0)
    for copy in copies:
        copy.wait()
    total = parts[0]
    for b in range(1, bands):
        total = total + parts[b]
    packed = total.astype(jnp.bfloat16)
    mine[...] = packed
    copies = []
    for d in range(1, slabs):
        copy = pltpu.make_async_remote_copy(
            src_ref=mine, dst_ref=rows.at[slab], send_sem=send_b.at[d - 1],
            recv_sem=recv_b.at[d - 1], device_id=slab_peer(d), device_id_type=mesh_id,
        )
        copy.start()
        copies.append(copy)
    rows[slab] = packed
    count = hot_ref.shape[0]
    plan_slots(slab, spots, count, count + 1, hot_ref, table_ref, counts_ref)
    for copy in copies:
        copy.wait()
    out_ref[...] = rows[...]
    shape_load.wait()


def share(coefficients, occupation, shapes, corners, bands, slabs):
    atoms, projectors, depth = coefficients.shape
    lines = atoms + atoms // 2
    slots = 4 * atoms
    f32 = jnp.float32
    vmem = pl.BlockSpec(memory_space=pltpu.VMEM)
    hbm = pl.BlockSpec(memory_space=pltpu.HBM)
    inputs = (jnp.transpose(coefficients, (1, 0, 2)), occupation.reshape(1, depth), shapes, corners)
    return pl.pallas_call(
        functools.partial(share_kernel, bands, slabs),
        out_shape=[
            pltpu.VMEM((slabs, lines, LANES), jnp.bfloat16),
            pltpu.VMEM((slots, corners.shape[1]), jnp.bfloat16),
            pltpu.VMEM((8, slots), jnp.int32),
            pltpu.VMEM((CHUNKS, LANES), jnp.int32),
            pltpu.VMEM(shapes.shape, shapes.dtype),
            pltpu.VMEM(((shapes.shape[1] // LANES + 2 * PAD) * (slots + 1), LANES), f32),
            *[pltpu.VMEM((CHUNKS * WINDOWS * NY, LANES), f32)] * DEEP,
        ],
        in_specs=[hbm] * 4,
        out_specs=[vmem] * (6 + DEEP),
        scratch_shapes=[
            pltpu.VMEM((projectors, atoms, depth), jnp.bfloat16),
            pltpu.VMEM((1, depth), jnp.int32),
            pltpu.VMEM(corners.shape, jnp.int32),
            pltpu.VMEM((projectors, atoms, depth), f32),
            pltpu.VMEM((lines, LANES), f32),
            pltpu.VMEM((bands, lines, LANES), f32),
            pltpu.VMEM((lines, LANES), jnp.bfloat16),
            pltpu.VMEM((slabs, lines, LANES), jnp.bfloat16),
            pltpu.SemaphoreType.DMA((3,)),
            pltpu.SemaphoreType.DMA,
            pltpu.SemaphoreType.DMA((bands - 1,)),
            pltpu.SemaphoreType.DMA((bands - 1,)),
            pltpu.SemaphoreType.DMA((slabs - 1,)),
            pltpu.SemaphoreType.DMA((slabs - 1,)),
        ],
        compiler_params=pltpu.CompilerParams(
            collective_id=0, has_side_effects=True, vmem_limit_bytes=6 * 1024 * 1024
        ),
    )(*[pltpu.with_memory_space_constraint(value, pltpu.HBM) for value in inputs])


def body(coefficients, occupation, shapes, corners):
    bands, slabs = lax.axis_size("band"), lax.axis_size("grid")
    packed, hot, table, counts, shapes, *sums = share(
        coefficients, occupation, shapes, corners, bands, slabs
    )
    return place_boxes(packed, hot, table, counts, shapes, sums, 2 * coefficients.shape[0])


def solution(mesh):
    placed = (P("grid", None, "band"), P("band"), P(), P())
    return jax.shard_map(
        body, mesh=mesh, in_specs=placed, out_specs=P("grid", None, None), check_vma=False
    )
```
